32 devices in a mesh: rep: 4 (over z), exp: 8 (over y, x, core).
Axes of the slice: x: 2, y: 2, z: 4, core: 2. Of those that a mesh axis runs over, the one named last changes fastest.
Arguments:
- tokens: bfloat16 [64, 128, 512], P('rep', 'exp'), may hold values from -48 to 48
- gate: float32 [64, 128], P('rep', 'exp'), may hold values from 0.25 to 1
- route: int32 [4, 8, 256, 1], P('rep', 'exp'), may hold values from 0 to 7; in each aligned block of 256 rows (0 to 255, 256 to 511, ..., all dimensions but the last counted through in order) at most 48 rows name the same one
- cotangent: bfloat16 [64, 128, 512], P('rep', 'exp'), may hold values from -6 to 6
- w_qkv: bfloat16 [512, 1536], replicated, may hold values from -1 to 1
- w_proj: bfloat16 [512, 512], replicated, may hold values from -0.25 to 0.25
- w_up: bfloat16 [8, 2048, 512], P('exp', 'rep'), may hold values from -0.25 to 0.25
- w_down: bfloat16 [8, 2048, 512], P('exp', 'rep'), may hold values from -0.125 to 0.125
Outputs:
- layer_out: bfloat16 [64, 128, 512], P('rep', 'exp')
- input_grad: bfloat16 [64, 128, 512], P('rep', 'exp')
- grad_up: float32 [8, 2048, 512], P('exp', 'rep')
- grad_down: float32 [8, 2048, 512], P('exp', 'rep')
The draws below stay inside these ranges and needn't reach their ends.
Inputs may be any that keep to these rules, and one draw needn't show every extreme that they name: `route`: among the tokens of one tile no expert is named more than 48 times.
All inputs are finite; a program needn't handle non-finite values.
Results may differ from the reference program's by a relative error of at most 0.018.
Values may be sent and summed in bfloat16 or wider, within the bound.
A program may use at most 64 MiB of HBM per device.

```python
import math
import jax
import jax.numpy as jnp
import numpy as np
from jax import lax

D = 512
FF = 2048
HEADS = 16
TROWS = 16
TCOLS = 16
EXPERTS = 8
TOK_DEV = 256
CAP = 48
ROWS = 64
COLS = 128
N_REP = 4
N_EXP = 8


def draw_tokens(key, part):
    key_base = jax.random.fold_in(jax.random.fold_in(key, 11), 0)
    base = jax.random.normal(key_base, (ROWS, COLS, D), jnp.float32)
    return jnp.clip(base, -48.0, 48.0).astype(jnp.bfloat16)


def draw_w_qkv(key, part):
    key_main = jax.random.fold_in(jax.random.fold_in(key, 23), 0)
    matrix = jnp.clip(jax.random.normal(key_main, (D, 3 * D), jnp.float32), -6.0, 6.0) / jnp.sqrt(jnp.float32(D))
    return matrix.astype(jnp.bfloat16)


def steps_of(key, extent, cuts, smallest, high):
    loudness, own = 1.0, jax.random.fold_in(key, 6)
    for dim, shards_of in cuts:
        draws = jnp.exp(jax.random.uniform(jax.random.fold_in(own, dim), (shards_of,), jnp.float32, smallest / len(cuts), high / len(cuts)))
        loudness = loudness * jnp.repeat(draws, extent[dim] // shards_of).reshape([-1 if axis == dim else 1 for axis in range(len(extent))])
    return loudness


def assign_block(own_key, own, number, rows, amount, top, limit, slope):
    ranking = jax.random.permutation(own_key, amount)
    packed, common = shares(amount, rows * top, limit, slope, True), shares(amount, rows * top, limit, slope, False)
    places = jnp.arange(amount)

    def named(sizes, offset_by):
        used = int((sizes > 0).sum())
        fixed = max(1, used // 4)
        shifted = fixed + (places - fixed + offset_by * (used - fixed)) % max(1, amount - fixed)
        return jnp.zeros((amount,), jnp.int32).at[ranking[jnp.where(places < fixed, places, shifted)]].set(jnp.asarray(sizes, jnp.int32))

    sizes = jnp.where(number % 4 == 0, named(packed, number // 4), named(common, number - number // 4 - 1))
    mixed = jax.random.permutation(jax.random.fold_in(own, 3), amount)
    source_of, receiver = mixed[0:amount // 2 * 2:2], mixed[1:amount // 2 * 2:2]
    margin = jnp.minimum(sizes[source_of] - 1, limit - sizes[receiver]) // 2
    margin = jnp.where((source_of == ranking[0]) | (receiver == ranking[0]) | (sizes[receiver] == 0), 0, jnp.maximum(margin, 0))
    shifted = jax.random.randint(jax.random.fold_in(own, 4), (amount // 2,), 0, 1 << 20) % (margin + 1)
    sizes = sizes.at[source_of].add(-shifted).at[receiver].add(shifted)
    members = jnp.searchsorted(jnp.cumsum(sizes), jnp.arange(rows * top), side="right").astype(jnp.int32)
    listing = members.reshape(top, rows).T
    listing = listing[jax.random.permutation(jax.random.fold_in(own, 1), rows)]
    offset_by = jax.random.randint(jax.random.fold_in(own, 2), (rows, 1), 0, top)
    return jnp.take_along_axis(listing, (jnp.arange(top)[None, :] + offset_by) % top, axis=1)


def shares(amount, total, most, lean, full):
    loads = [(1 << 20) // math.isqrt(rank ** lean) + 1 for rank in range(1, amount + 1)]
    largest = most if full else min(most, max(-(-total // amount), total * loads[0] // sum(loads)))
    least = 1 if total - largest >= amount - 1 else 0
    holding, rest = [largest] + [least] * (amount - 1), total - largest - least * (amount - 1)
    while rest > 0:
        movable = [i for i in range(1, amount) if holding[i] < largest] or [i for i in range(1, amount) if holding[i] < most]
        pool, remaining = sum([loads[i] for i in movable]), rest
        for i in movable:
            addition = min(most - holding[i], max(1, remaining * loads[i] // pool), rest)
            holding[i] = holding[i] + addition
            rest = rest - addition
    return np.array(holding)


def normal_values(own_key, shape, width, most, cuts=(), kind=jnp.bfloat16):
    gain = steps_of(own_key, shape, cuts, -0.22, 0.18) if cuts else 1.0
    result = jax.random.normal(own_key, shape, jnp.float32) * width * gain
    return jnp.minimum(jnp.maximum(result, -most), most).astype(kind)


def setup_inputs(seed: int = 0) -> dict:
    splits = jax.random.split(jax.random.key(seed), 9)
    tokens = draw_tokens(jax.random.fold_in(splits[8], 71), 0)
    gate = jnp.clip(0.25 + 0.75 * jax.random.uniform(splits[1], (ROWS, COLS), jnp.float32) ** steps_of(splits[1], (ROWS, COLS), ((0, 4), (1, 8)), -0.2, 0.2), 0.25, 1.0)
    route_keys = jax.random.split(jax.random.fold_in(splits[2], 1), N_REP * N_EXP * TOK_DEV // TOK_DEV)
    route_turns = jax.random.permutation(jax.random.fold_in(splits[2], 3), N_REP * N_EXP * TOK_DEV // TOK_DEV)
    route = jax.vmap(lambda own, number: assign_block(jax.random.fold_in(splits[2], 2), own, number, TOK_DEV, EXPERTS, 1, CAP, 2))(route_keys, route_turns).reshape((N_REP, N_EXP, TOK_DEV, 1))
    cotangent = normal_values(splits[3], (ROWS, COLS, D), 1.0, 6.0, ((0, 4), (1, 8)))
    w_qkv = draw_w_qkv(jax.random.fold_in(splits[8], 71), 0)
    w_proj = normal_values(splits[5], (D, D), D ** -0.5, 0.25)
    w_up = normal_values(splits[6], (EXPERTS, FF, D), D ** -0.5, 0.25, ((0, 8), (1, 4)))
    w_down = normal_values(splits[7], (EXPERTS, FF, D), FF ** -0.5, 0.125, ((0, 8), (1, 4)))
    return {"tokens": tokens, "gate": gate, "route": route, "cotangent": cotangent, "w_qkv": w_qkv, "w_proj": w_proj, "w_up": w_up, "w_down": w_down}


GELU_C = math.sqrt(2.0 / math.pi)
window_side = 8
margin_cells = 4

def gelu_tanh(inputs):
    return 0.5 * inputs * (1.0 + jnp.tanh(GELU_C * (inputs + 0.044715 * inputs * inputs * inputs)))

def gelu_slope(inputs):
    inner = jnp.tanh(GELU_C * (inputs + 0.044715 * inputs * inputs * inputs))
    return 0.5 * (1.0 + inner) + 0.5 * inputs * (1.0 - inner * inner) * GELU_C * (1.0 + 3.0 * 0.044715 * inputs * inputs)

def layer_norm(values):
    average = lax.optimization_barrier(jnp.mean(values, axis=-1, keepdims=True))
    centred = values - average
    spread = lax.optimization_barrier(jnp.mean(centred * centred, axis=-1, keepdims=True))
    return centred * lax.rsqrt(spread + 1e-05)

def window_attend(qkv, in_grid):
    ext_rows, ext_cols, triple = qkv.shape
    feature = triple // 3
    head_size = feature // HEADS
    win_rows = ext_rows // window_side
    win_cols = ext_cols // window_side
    cells = window_side * window_side
    blocks = qkv.reshape(win_rows, window_side, win_cols, window_side, triple).transpose(0, 2, 1, 3, 4)
    blocks = blocks.reshape(win_rows * win_cols, cells, 3, HEADS, head_size)
    present = in_grid.reshape(win_rows, window_side, win_cols, window_side).transpose(0, 2, 1, 3).reshape(win_rows * win_cols, cells)
    queries = blocks[:, :, 0].astype(jnp.float32)
    key_part = blocks[:, :, 1].astype(jnp.float32)
    value_part = blocks[:, :, 2].astype(jnp.float32)
    scores = jnp.einsum('wqhd,wkhd->whqk', queries, key_part) / math.sqrt(head_size)
    scores = jnp.where(present[:, None, None, :], scores, jnp.float32(-1e+30))
    peak_score = lax.optimization_barrier(jnp.max(scores, axis=-1, keepdims=True))
    weights = jnp.exp(scores - peak_score)
    probabilities = (weights / lax.optimization_barrier(jnp.sum(weights, axis=-1, keepdims=True))).astype(jnp.bfloat16)
    context = jnp.einsum('whqk,wkhd->wqhd', probabilities.astype(jnp.float32), value_part).astype(jnp.bfloat16)
    context = context.reshape(win_rows, win_cols, window_side, window_side, feature).transpose(0, 2, 1, 3, 4)
    return context.reshape(ext_rows, ext_cols, feature)

def to_devices(values):
    return values.reshape(N_REP, TROWS, N_EXP, TCOLS, -1).transpose(0, 2, 1, 3, 4).reshape(N_REP, N_EXP, TOK_DEV, -1)

def to_grid(values):
    return values.reshape(N_REP, N_EXP, TROWS, TCOLS, -1).transpose(0, 2, 1, 3, 4).reshape(N_REP * TROWS, N_EXP * TCOLS, -1)

def one_replica(slot_rows, slot_grads, up_mat, down_mat):
    pre_act = jnp.dot(slot_rows, up_mat.T, preferred_element_type=jnp.float32)
    hidden = gelu_tanh(pre_act).astype(jnp.bfloat16)
    expert_out = jnp.dot(hidden, down_mat, preferred_element_type=jnp.float32).astype(jnp.bfloat16)
    hidden_grad = jnp.dot(slot_grads, down_mat.T, preferred_element_type=jnp.float32)
    pre_grad = (hidden_grad * gelu_slope(pre_act)).astype(jnp.bfloat16)
    input_slots = jnp.dot(pre_grad, up_mat, preferred_element_type=jnp.float32).astype(jnp.bfloat16)
    part_up = jnp.dot(pre_grad.T, slot_rows, preferred_element_type=jnp.float32).astype(jnp.bfloat16)
    part_down = jnp.dot(hidden.T, slot_grads, preferred_element_type=jnp.float32).astype(jnp.bfloat16)
    return (expert_out, input_slots, part_up, part_down)

def one_expert(operands):
    rows_all, grads_all, up_mat, down_mat = operands
    expert_out, input_slots, part_up, part_down = jax.vmap(one_replica, in_axes=(0, 0, None, None))(rows_all, grads_all, up_mat, down_mat)
    grad_up = lax.optimization_barrier(jnp.sum(part_up.astype(jnp.float32), axis=0)) / N_REP
    grad_down = lax.optimization_barrier(jnp.sum(part_down.astype(jnp.float32), axis=0)) / N_REP
    return (expert_out, input_slots, grad_up, grad_down)

def reference(tokens, gate, route, cotangent, w_qkv, w_proj, w_up, w_down):
    grid_rows, grid_cols, feature = tokens.shape
    padded = jnp.pad(tokens, ((margin_cells, margin_cells), (margin_cells, margin_cells), (0, 0)))
    ext_rows = grid_rows + 2 * margin_cells
    ext_cols = grid_cols + 2 * margin_cells
    qkv_all = jnp.dot(padded.reshape(-1, feature), w_qkv, preferred_element_type=jnp.float32).astype(jnp.bfloat16)
    qkv_all = qkv_all.reshape(ext_rows, ext_cols, 3 * feature)
    row_ids = jnp.arange(ext_rows, dtype=jnp.int32) - margin_cells
    col_ids = jnp.arange(ext_cols, dtype=jnp.int32) - margin_cells
    in_grid = ((row_ids >= 0) & (row_ids < grid_rows))[:, None] & ((col_ids >= 0) & (col_ids < grid_cols))[None, :]
    context = window_attend(qkv_all, in_grid)[margin_cells:grid_rows + margin_cells, margin_cells:grid_cols + margin_cells].reshape(-1, feature)
    attended = jnp.dot(context, w_proj, preferred_element_type=jnp.float32)
    mixed = (tokens.reshape(-1, feature).astype(jnp.float32) + layer_norm(attended)).astype(jnp.bfloat16)
    mixed_dev = to_devices(mixed.reshape(grid_rows, grid_cols, feature))
    gate_dev = to_devices(gate[:, :, None])[..., 0]
    upstream = (gate[:, :, None] * cotangent.astype(jnp.float32)).astype(jnp.bfloat16)
    upstream_dev = to_devices(upstream)
    chosen = route[..., 0]
    matches = (chosen[..., None] == jnp.arange(EXPERTS, dtype=jnp.int32)).astype(jnp.int32)
    position = lax.optimization_barrier(jnp.sum(matches * (jnp.cumsum(matches, axis=2) - 1), axis=-1)).astype(jnp.int32)
    replica = jnp.arange(N_REP, dtype=jnp.int32)[:, None, None]
    source = jnp.arange(N_EXP, dtype=jnp.int32)[None, :, None]
    target = (((replica * EXPERTS + chosen) * N_EXP + source) * CAP + position).reshape(-1).astype(jnp.int32)
    total = N_REP * EXPERTS * N_EXP * CAP
    slots_x = jnp.zeros((total, feature), jnp.bfloat16).at[target].set(mixed_dev.reshape(-1, feature))
    slots_g = jnp.zeros((total, feature), jnp.bfloat16).at[target].set(upstream_dev.reshape(-1, feature))
    slots_x = slots_x.reshape(N_REP, EXPERTS, N_EXP * CAP, feature).transpose(1, 0, 2, 3)
    slots_g = slots_g.reshape(N_REP, EXPERTS, N_EXP * CAP, feature).transpose(1, 0, 2, 3)
    expert_out, input_slots, grad_up, grad_down = lax.map(one_expert, (slots_x, slots_g, w_up, w_down))
    out_flat = expert_out.transpose(1, 0, 2, 3).reshape(total, feature)
    back_flat = input_slots.transpose(1, 0, 2, 3).reshape(total, feature)
    out_tok = out_flat[target].reshape(N_REP, N_EXP, TOK_DEV, feature).astype(jnp.float32)
    grad_tok = back_flat[target].reshape(N_REP, N_EXP, TOK_DEV, feature)
    layer_dev = (mixed_dev.astype(jnp.float32) + gate_dev[..., None] * out_tok).astype(jnp.bfloat16)
    return (to_grid(layer_dev), to_grid(grad_tok), grad_up, grad_down)
```

```python
import math

import jax
import jax.numpy as jnp
import numpy as np
from jax import lax
from jax.experimental import pallas as pl
from jax.experimental.pallas import tpu as pltpu
from jax.sharding import PartitionSpec as P

HEADS = 16
GELU_C = math.sqrt(2.0 / math.pi)
window_side = 8
margin_cells = 4
PAIR = 2
f32, bf16 = jnp.float32, jnp.bfloat16


class Windows:
    def __init__(self, tile_rows, tile_cols):
        def cut(size):
            parts = [margin_cells] + [window_side] * ((size - 2 * margin_cells) // window_side)
            return parts + [margin_cells]

        self.heights, self.widths = cut(tile_rows), cut(tile_cols)
        self.cells = window_side * window_side
        self.wins, start = [], 0
        position = np.zeros((tile_rows, tile_cols), np.int32)
        top = 0
        for i, h in enumerate(self.heights):
            left = 0
            for j, w in enumerate(self.widths):
                position[top : top + h, left : left + w] = start + np.arange(h * w).reshape(h, w)
                sizes = (h * w, (window_side - h) * w, h * (window_side - w), (window_side - h) * (window_side - w))
                self.wins.append((i, j, start, sizes))
                start += h * w
                left += w
            top += h
        self.position = position.reshape(-1)
        self.last = (len(self.heights) - 1, len(self.widths) - 1)

    def number(self, i, j):
        return i * len(self.widths) + j

    def segment(self, number, kind):
        sizes = self.wins[number][3]
        return number * self.cells + sum(sizes[:kind]), sizes[kind]

    def pieces(self, dv, dh):
        found = []
        for number, (i, j, _, _) in enumerate(self.wins):
            vertical = (dv == -1 and i == 0) or (dv == 1 and i == self.last[0])
            beside = (dh == -1 and j == 0) or (dh == 1 and j == self.last[1])
            if (dv and not vertical) or (dh and not beside):
                continue
            kind = (1 if dv else 0) + (2 if dh else 0)
            theirs = self.number(self.last[0] - i if dv else i, self.last[1] - j if dh else j)
            place, rows = self.segment(number, kind)
            found.append((self.wins[theirs][2], place, rows))
        return found


SIDES = [(v, h) for v in (-1, 0, 1) for h in (-1, 0, 1) if (v, h) != (0, 0)]


def each(begin, end, body):
    if end - begin == 1:
        body(begin)
    elif end > begin:
        lax.fori_loop(begin, end, lambda k, carry: (body(k), carry)[1], 0)


def drain(ref, sem):
    pltpu.make_async_copy(ref, ref, sem).wait()


def dot_t(a, b):
    return lax.dot_general(a, b, (((1,), (1,)), ((), ())), preferred_element_type=f32)


def t_dot(a, b):
    return lax.dot_general(a, b, (((0,), (0,)), ((), ())), preferred_element_type=f32)


def dot(a, b):
    return jnp.dot(a, b, preferred_element_type=f32)


def layer_norm(values):
    average = jnp.mean(values, axis=-1, keepdims=True)
    centred = values - average
    spread = jnp.mean(centred * centred, axis=-1, keepdims=True)
    return centred * lax.rsqrt(spread + 1e-05)


def layer_kernel(
    wins, ring, ranks, cap, tile_cols,
    tokens, cotangent, gate, route, position, w_qkv_hbm, w_proj_hbm, w_up_hbm, w_down_hbm,
    layer_out, input_grad, grad_up, grad_down,
    w_qkv, w_proj, w_up, w_down, grouped, ext, kv, queries, context, mixed, upstream, gate_col,
    marks, placers, held, slots, gathered, hidden, pre_grad, parts, back, sums, arrived, share, taken,
    load_sem, halo_send, halo_recv, mark_send, mark_recv, z_send, z_recv, a_send, a_recv,
    b_send, b_recv, w_send, w_recv, r_send, r_recv, g_send, g_recv,
):
    me, row = lax.axis_index("exp"), lax.axis_index("rep")
    tok, feature = tokens.shape
    units = w_up.shape[1]
    tiles = ranks // PAIR
    buddy = row + 1 - 2 * lax.rem(row, 2)
    head_size = feature // HEADS

    def partner(j):
        return lax.rem(row + PAIR * j, ranks)

    loads = [
        pltpu.make_async_copy(source, target, load_sem.at[i])
        for i, (source, target) in enumerate(
            ((w_up_hbm, w_up.at[0]), (w_down_hbm, w_down.at[0]), (w_qkv_hbm, w_qkv), (w_proj_hbm, w_proj))
        )
    ]
    for load in loads:
        load.start()

    barrier = pltpu.get_barrier_semaphore()

    def near(v, h):
        conds = []
        if v:
            conds.append((row + v >= 0) & (row + v < ranks))
        if h:
            conds.append((me + h >= 0) & (me + h < ring))
        return conds[0] if len(conds) == 1 else conds[0] & conds[1]

    def greet_ring(step, carry):
        pl.semaphore_signal(barrier, device_id={"exp": lax.rem(me + step, ring)})
        return carry

    def greet_ranks(step, carry):
        pl.semaphore_signal(barrier, device_id={"rep": lax.rem(row + step, ranks)})
        return carry

    lax.fori_loop(1, ring, greet_ring, 0)
    lax.fori_loop(1, ranks, greet_ranks, 0)
    for v, h in SIDES:
        if v and h:
            @pl.when(near(v, h))
            def _():
                pl.semaphore_signal(barrier, device_id={"rep": row + v, "exp": me + h})

    spots = position[0:1, :]
    perm = (lax.broadcasted_iota(jnp.int32, (tok, tok), 0) == spots).astype(f32).astype(bf16)
    grouped[...] = dot(perm, tokens[...]).astype(bf16)
    for number, (i, j, start, sizes) in enumerate(wins.wins):
        ext[pl.ds(number * wins.cells, sizes[0]), :] = grouped[pl.ds(start, sizes[0]), :]
    for v, h in SIDES:
        @pl.when(jnp.logical_not(near(v, h)))
        def _():
            for _, place, rows in wins.pieces(v, h):
                ext[pl.ds(place, rows), :] = jnp.zeros((rows, feature), bf16)

    down = (row + ranks - 1) // ranks + (2 * ranks - 2 - row) // ranks
    across = (me + ring - 1) // ring + (2 * ring - 2 - me) // ring
    pl.semaphore_wait(barrier, ring - 1 + ranks - 1 + down * across)

    for index, (v, h) in enumerate(SIDES):
        @pl.when(near(v, h))
        def _():
            device = {"rep": row + v} if not h else {"exp": me + h} if not v else {"rep": row + v, "exp": me + h}
            for source, place, rows in wins.pieces(-v, -h):
                pltpu.make_async_remote_copy(
                    src_ref=grouped.at[pl.ds(source, rows)],
                    dst_ref=ext.at[pl.ds(place, rows)],
                    send_sem=halo_send.at[index],
                    recv_sem=halo_recv.at[len(SIDES) - 1 - index],
                    device_id=device,
                ).start()

    lanes = max(8, ring)
    routes = route[0:1, :].astype(f32)
    match = (lax.broadcasted_iota(jnp.int32, (lanes, tok), 0).astype(f32) == routes).astype(f32)
    before = (
        lax.broadcasted_iota(jnp.int32, (tok, tok), 0) < lax.broadcasted_iota(jnp.int32, (tok, tok), 1)
    ).astype(f32).astype(bf16)
    earlier = dot(match.astype(bf16), before)
    ids = routes * cap + jnp.sum(match * earlier, axis=0, keepdims=True)
    marks[0] = jnp.broadcast_to(ids.astype(jnp.int32), marks.shape[1:])

    def send_marks(j):
        pltpu.make_async_remote_copy(
            src_ref=marks.at[0],
            dst_ref=marks.at[tiles - j],
            send_sem=mark_send.at[j],
            recv_sem=mark_recv.at[tiles - j],
            device_id={"rep": partner(j)},
        ).start()

    def send_tokens(t, source, j):
        pltpu.make_async_remote_copy(
            src_ref=source,
            dst_ref=held.at[t, tiles - j],
            send_sem=z_send.at[t, j],
            recv_sem=z_recv.at[t, tiles - j],
            device_id={"rep": partner(j)},
        ).start()

    def make_placer(j):
        slot_ids = lax.broadcasted_iota(jnp.int32, placers.shape[1:], 0)
        placers[j] = (slot_ids == marks[j, 0:1, :]).astype(f32).astype(bf16)

    def swap(source, target, send_sem, recv_sem):
        mine = pl.ds(pl.multiple_of(me * cap, 16), cap)

        def send(step, carry):
            peer = lax.rem(me + step, ring)
            pltpu.make_async_remote_copy(
                src_ref=source.at[pl.ds(pl.multiple_of(peer * cap, 16), cap)],
                dst_ref=target.at[mine],
                send_sem=send_sem,
                recv_sem=recv_sem,
                device_id={"exp": peer},
            ).start()
            return carry

        lax.fori_loop(1, ring, send, 0)
        pltpu.make_async_copy(source.at[mine], target.at[mine], recv_sem).start()

    def dispatch(t, j, values):
        slots[t, j] = dot(placers[j], values).astype(bf16)
        swap(slots.at[t, j], gathered.at[t, j], a_send.at[t, j], a_recv.at[t, j])

    each(1, tiles, send_marks)
    grid_row = lax.broadcasted_iota(jnp.int32, (tok, gate.shape[0]), 0) // tile_cols
    picks = (grid_row == lax.broadcasted_iota(jnp.int32, (tok, gate.shape[0]), 1)).astype(f32)
    gate_rows = lax.dot_general(
        picks, gate[...], (((1,), (0,)), ((), ())), precision=lax.Precision.HIGHEST, preferred_element_type=f32
    )
    grid_col = lax.rem(lax.broadcasted_iota(jnp.int32, (tok, tile_cols), 0), tile_cols)
    chosen = jnp.where(grid_col == lax.broadcasted_iota(jnp.int32, (tok, tile_cols), 1), gate_rows, 0.0)
    gate_col[...] = jnp.broadcast_to(jnp.sum(chosen, axis=1, keepdims=True), gate_col.shape)
    upstream[...] = (gate_col[:, 0:1] * cotangent[...].astype(f32)).astype(bf16)
    each(1, tiles, lambda j: send_tokens(0, upstream, j))
    make_placer(0)
    dispatch(0, 0, upstream[...])

    def send_weight(index, source, target):
        loads[index].wait()
        pltpu.make_async_remote_copy(
            src_ref=source,
            dst_ref=target,
            send_sem=w_send.at[index],
            recv_sem=w_recv.at[index],
            device_id={"rep": buddy},
        ).start()

    send_weight(0, w_up.at[0], w_up.at[1])
    send_weight(1, w_down.at[0], w_down.at[1])

    loads[2].wait()
    queries[...] = dot(grouped[...], w_qkv[:, :feature]).astype(bf16)
    for index, (v, h) in enumerate(SIDES):
        @pl.when(near(v, h))
        def _():
            amount = sum(rows for _, _, rows in wins.pieces(v, h))
            drain(grouped.at[pl.ds(0, amount)], halo_recv.at[index])

    kv[...] = dot(ext[...], w_qkv[:, feature:]).astype(bf16)
    key_lane = lax.broadcasted_iota(jnp.int32, (1, wins.cells), 1)
    group = 128 // head_size

    def attend(number):
        i, j, start, sizes = wins.wins[number]
        amount = sizes[0]
        absent = jnp.zeros((1, wins.cells), f32)
        v = -1 if i == 0 else 1 if i == wins.last[0] else 0
        h = -1 if j == 0 else 1 if j == wins.last[1] else 0
        for side in {(v, 0), (0, h), (v, h)} - {(0, 0)}:
            kind = (1 if side[0] else 0) + (2 if side[1] else 0)
            first = sum(sizes[:kind])
            inside = (key_lane >= first) & (key_lane < first + sizes[kind])
            missing = jnp.where(near(*side), 0.0, -1e30)
            absent = jnp.where(inside, missing, absent)
        lane = lax.broadcasted_iota(jnp.int32, (amount, 128), 1)
        keep = [((lane >= g * head_size) & (lane < (g + 1) * head_size)).astype(f32) for g in range(group)]
        mine, theirs = pl.ds(start, amount), pl.ds(number * wins.cells, wins.cells)
        for first in range(0, feature, 128):
            query = queries[mine, pl.ds(first, 128)]
            stacked = jnp.concatenate([query * k.astype(bf16) for k in keep], axis=0)
            scores = dot_t(stacked, kv[theirs, pl.ds(first, 128)]) * (1.0 / math.sqrt(head_size)) + absent
            weights = jnp.exp(scores - jnp.max(scores, axis=-1, keepdims=True))
            total = jnp.sum(weights, axis=-1, keepdims=True)
            probs = (weights * (1.0 / total)).astype(bf16)
            found = dot(probs, kv[theirs, pl.ds(feature + first, 128)])
            picked = sum(k * found[g * amount : (g + 1) * amount] for g, k in enumerate(keep))
            context[mine, pl.ds(first, 128)] = picked.astype(bf16)

    def bring(t, j):
        if t == 0:
            drain(marks.at[0], mark_recv.at[j])
            make_placer(j)
        drain(held.at[t, j], z_recv.at[t, j])
        dispatch(t, j, held[t, j])

    count = len(wins.wins)
    for number in range(count // 2):
        attend(number)
    each(1, tiles, lambda j: bring(0, j))
    for number in range(count // 2, count):
        attend(number)

    loads[3].wait()
    attended = dot(context[...], w_proj[...])
    blended = (grouped[...].astype(f32) + layer_norm(attended)).astype(bf16)
    mixed[...] = t_dot(perm, blended).astype(bf16)
    each(1, tiles, lambda j: send_tokens(1, mixed, j))
    dispatch(1, 0, mixed[...])

    def arrive(t, j):
        drain(gathered.at[t, j], a_recv.at[t, j])

    block = min(256, units)

    def experts(j):
        arrive(0, j)
        arrive(1, j)
        for half in range(PAIR):
            for first in range(0, units, block):
                spot = pl.ds(half * units + first, block)
                up, low = w_up[half, pl.ds(first, block), :], w_down[half, pl.ds(first, block), :]
                pre = dot_t(gathered[1, j], up)
                flow = dot_t(gathered[0, j], low)
                square = pre * pre
                inner = jnp.tanh(GELU_C * (pre + 0.044715 * square * pre))
                hidden[j, :, spot] = (0.5 * pre * (1.0 + inner)).astype(bf16)
                slope = 0.5 * (1.0 + inner) + 0.5 * pre * (1.0 - inner * inner) * GELU_C * (
                    1.0 + 3.0 * 0.044715 * square
                )
                pre_grad[j, :, spot] = (flow * slope).astype(bf16)
        for t, (left, right) in enumerate(((hidden, w_down), (pre_grad, w_up))):
            total = dot(left[j, :, pl.ds(0, units)], right[0])
            for half in range(1, PAIR):
                total += dot(left[j, :, pl.ds(half * units, units)], right[half])
            parts[t, j] = total.astype(bf16)
            swap(parts.at[t, j], back.at[t, j], b_send.at[t, j], b_recv.at[t, j])

    for index, weight in enumerate((w_up, w_down)):
        drain(weight.at[1], w_recv.at[index])
    experts(0)
    each(1, tiles, lambda j: bring(1, j))
    each(1, tiles, experts)

    rows = tiles * hidden.shape[1]

    def gradient(t, half):
        left = (pre_grad, hidden)[t][...].reshape(rows, PAIR * units)[:, half * units : (half + 1) * units]
        return t_dot(left, gathered[1 - t].reshape(rows, feature))

    for t in range(2):
        share[t] = gradient(t, 1).astype(bf16)
        pltpu.make_async_remote_copy(
            src_ref=share.at[t],
            dst_ref=taken.at[t],
            send_sem=g_send.at[t],
            recv_sem=g_recv.at[t],
            device_id={"rep": buddy},
        ).start()

    def placed(t, j):
        drain(back.at[t, j], b_recv.at[t, j])
        return t_dot(placers[j], back[t, j])

    def give(j):
        for t in range(2):
            sums[t, j] = placed(t, j).astype(bf16)
            pltpu.make_async_remote_copy(
                src_ref=sums.at[t, j],
                dst_ref=arrived.at[t, tiles - j],
                send_sem=r_send.at[t, j],
                recv_sem=r_recv.at[t, tiles - j],
                device_id={"rep": partner(j)},
            ).start()

    each(1, tiles, give)
    grad_up[...] = gradient(0, 0)
    grad_down[...] = gradient(1, 0)

    def total_of(t):
        value = placed(t, 0)
        for j in range(1, tiles):
            drain(arrived.at[t, j], r_recv.at[t, j])
            value += arrived[t, j].astype(f32)
        return value

    layer_out[...] = (mixed[...].astype(f32) + gate_col[:, 0:1] * total_of(0)).astype(bf16)
    input_grad[...] = total_of(1).astype(bf16)
    factor = 1.0 / ranks
    for t, out in enumerate((grad_up, grad_down)):
        drain(taken.at[t], g_recv.at[t])
        out[...] = (out[...] + taken[t].astype(f32)) * factor

    for index, (v, h) in enumerate(SIDES):
        @pl.when(near(v, h))
        def _():
            amount = sum(rows for _, _, rows in wins.pieces(-v, -h))
            drain(grouped.at[pl.ds(0, amount)], halo_send.at[index])

    for t in range(2):
        drain(w_up.at[0], w_send.at[t])
        drain(share.at[t], g_send.at[t])

    def finish(j):
        for t in range(2):
            sent = slots.at[t, j, pl.ds(0, (ring - 1) * cap)]
            drain(sent, a_send.at[t, j])
            drain(sent, b_send.at[t, j])

    each(0, tiles, finish)

    def finish_far(j):
        drain(marks.at[0], mark_send.at[j])
        for t in range(2):
            drain(mixed, z_send.at[t, j])
            drain(mixed, r_send.at[t, j])

    each(1, tiles, finish_far)


def per_device(ranks, ring, tokens, gate, route, cotangent, w_qkv, w_proj, w_up, w_down):
    tile_rows, tile_cols, feature = tokens.shape
    tok = tile_rows * tile_cols
    units = w_up.shape[1]
    capacity = max(2, 3 * tok // (2 * ring))
    capacity = -(-capacity // 16) * 16
    rows = ring * capacity
    tiles = ranks // PAIR
    wins = Windows(tile_rows, tile_cols)
    ext = len(wins.wins) * wins.cells
    position = jnp.asarray(np.broadcast_to(wins.position[None, :], (8, tok)))

    def body(*refs):
        layer_kernel(wins, ring, ranks, capacity, tile_cols, *refs)

    vmem, anywhere = pl.BlockSpec(memory_space=pltpu.VMEM), pl.BlockSpec(memory_space=pl.ANY)
    dma = pltpu.SemaphoreType.DMA
    layer_out, input_grad, grad_up, grad_down = pl.pallas_call(
        body,
        name="layer",
        out_shape=(
            jax.ShapeDtypeStruct((tok, feature), bf16),
            jax.ShapeDtypeStruct((tok, feature), bf16),
            jax.ShapeDtypeStruct((units, feature), f32),
            jax.ShapeDtypeStruct((units, feature), f32),
        ),
        in_specs=[vmem] * 5 + [anywhere] * 4,
        out_specs=(vmem,) * 4,
        scratch_shapes=[
            pltpu.VMEM(w_qkv.shape, bf16),
            pltpu.VMEM(w_proj.shape, bf16),
            pltpu.VMEM((PAIR, units, feature), bf16),
            pltpu.VMEM((PAIR, units, feature), bf16),
            pltpu.VMEM((tok, feature), bf16),
            pltpu.VMEM((ext, feature), bf16),
            pltpu.VMEM((ext, 2 * feature), bf16),
            pltpu.VMEM((tok, feature), bf16),
            pltpu.VMEM((tok, feature), bf16),
            pltpu.VMEM((tok, feature), bf16),
            pltpu.VMEM((tok, feature), bf16),
            pltpu.VMEM((tok, 128), f32),
            pltpu.VMEM((tiles, 8, tok), jnp.int32),
            pltpu.VMEM((tiles, rows, tok), bf16),
            pltpu.VMEM((2, tiles, tok, feature), bf16),
            pltpu.VMEM((2, tiles, rows, feature), bf16),
            pltpu.VMEM((2, tiles, rows, feature), bf16),
            pltpu.VMEM((tiles, rows, PAIR * units), bf16),
            pltpu.VMEM((tiles, rows, PAIR * units), bf16),
            pltpu.VMEM((2, tiles, rows, feature), bf16),
            pltpu.VMEM((2, tiles, rows, feature), bf16),
            pltpu.VMEM((2, tiles, tok, feature), bf16),
            pltpu.VMEM((2, tiles, tok, feature), bf16),
            pltpu.VMEM((2, units, feature), bf16),
            pltpu.VMEM((2, units, feature), bf16),
            dma((4,)),
            dma((len(SIDES),)),
            dma((len(SIDES),)),
            dma((tiles,)),
            dma((tiles,)),
            dma((2, tiles)),
            dma((2, tiles)),
            dma((2, tiles)),
            dma((2, tiles)),
            dma((2, tiles)),
            dma((2, tiles)),
            dma((2,)),
            dma((2,)),
            dma((2, tiles)),
            dma((2, tiles)),
            dma((2,)),
            dma((2,)),
        ],
        compiler_params=pltpu.CompilerParams(
            collective_id=0, has_side_effects=True, vmem_limit_bytes=60 << 20
        ),
    )(
        tokens.reshape(tok, feature),
        cotangent.reshape(tok, feature),
        gate,
        route.reshape(1, tok),
        position,
        w_qkv,
        w_proj,
        w_up[0],
        w_down[0],
    )
    return (
        layer_out.reshape(tile_rows, tile_cols, feature),
        input_grad.reshape(tile_rows, tile_cols, feature),
        grad_up[None],
        grad_down[None],
    )


def solution(mesh):
    ranks, ring = mesh.shape["rep"], mesh.shape["exp"]
    placed = (
        P("rep", "exp", None),
        P("rep", "exp"),
        P("rep", "exp", None, None),
        P("rep", "exp", None),
        P(),
        P(),
        P("exp", "rep", None),
        P("exp", "rep", None),
    )

    def device(*arrays):
        return per_device(ranks, ring, *arrays)

    return jax.shard_map(
        device,
        mesh=mesh,
        in_specs=placed,
        out_specs=(
            P("rep", "exp", None),
            P("rep", "exp", None),
            P("exp", "rep", None),
            P("exp", "rep", None),
        ),
        check_vma=False,
    )
```

```python
import math

import jax
import jax.numpy as jnp
import numpy as np
from jax import lax
from jax.experimental import pallas as pl
from jax.experimental.pallas import tpu as pltpu
from jax.sharding import PartitionSpec as P

HEADS = 16
GELU_C = math.sqrt(2.0 / math.pi)
window_side = 8
margin_cells = 4
PAIR = 2
f32, bf16 = jnp.float32, jnp.bfloat16


class Windows:
    def __init__(self, tile_rows, tile_cols):
        def cut(size):
            parts = [margin_cells] + [window_side] * ((size - 2 * margin_cells) // window_side)
            return parts + [margin_cells]

        self.heights, self.widths = cut(tile_rows), cut(tile_cols)
        self.cells = window_side * window_side
        self.wins, start = [], 0
        for i, h in enumerate(self.heights):
            for j, w in enumerate(self.widths):
                sizes = (h * w, (window_side - h) * w, h * (window_side - w), (window_side - h) * (window_side - w))
                self.wins.append((i, j, start, sizes))
                start += h * w
        self.last = (len(self.heights) - 1, len(self.widths) - 1)

    def spots(self, tile_cols, tok):
        lane = lax.broadcasted_iota(jnp.int32, (1, tok), 1)
        rows, cols = lane // tile_cols, lax.rem(lane, tile_cols)

        def within(line, sizes):
            first, size, top = jnp.zeros_like(line), jnp.full_like(line, sizes[0]), 0
            for before, here in zip(sizes, sizes[1:]):
                top += before
                first, size = jnp.where(line >= top, top, first), jnp.where(line >= top, here, size)
            return first, size

        (top, height), (left, width) = within(rows, self.heights), within(cols, self.widths)
        return top * tile_cols + left * height + (rows - top) * width + cols - left

    def number(self, i, j):
        return i * len(self.widths) + j

    def segment(self, number, kind):
        sizes = self.wins[number][3]
        return number * self.cells + sum(sizes[:kind]), sizes[kind]

    def pieces(self, dv, dh):
        found = []
        for number, (i, j, _, _) in enumerate(self.wins):
            vertical = (dv == -1 and i == 0) or (dv == 1 and i == self.last[0])
            beside = (dh == -1 and j == 0) or (dh == 1 and j == self.last[1])
            if (dv and not vertical) or (dh and not beside):
                continue
            kind = (1 if dv else 0) + (2 if dh else 0)
            theirs = self.number(self.last[0] - i if dv else i, self.last[1] - j if dh else j)
            place, rows = self.segment(number, kind)
            found.append((self.wins[theirs][2], place, rows))
        return found


SIDES = [(v, h) for v in (-1, 0, 1) for h in (-1, 0, 1) if (v, h) != (0, 0)]


def each(begin, end, body):
    if end - begin == 1:
        body(begin)
    elif end > begin:
        lax.fori_loop(begin, end, lambda k, carry: (body(k), carry)[1], 0)


def drain(ref, sem):
    pltpu.make_async_copy(ref, ref, sem).wait()


def dot_t(a, b):
    return lax.dot_general(a, b, (((1,), (1,)), ((), ())), preferred_element_type=f32)


def t_dot(a, b):
    return lax.dot_general(a, b, (((0,), (0,)), ((), ())), preferred_element_type=f32)


def dot(a, b):
    return jnp.dot(a, b, preferred_element_type=f32)


def layer_norm(values):
    average = jnp.mean(values, axis=-1, keepdims=True)
    centred = values - average
    spread = jnp.mean(centred * centred, axis=-1, keepdims=True)
    return centred * lax.rsqrt(spread + 1e-05)


def layer_kernel(
    wins, ring, ranks, cap, tile_cols,
    tokens, cotangent, gate, route, w_qkv_hbm, w_proj_hbm, w_up_hbm, w_down_hbm,
    layer_out, input_grad, grad_up, grad_down,
    w_qkv, w_proj, w_up, w_down, grouped, ext, kv, queries, context, mixed, upstream, gate_col,
    marks, placers, held, slots, gathered, hidden, pre_grad, parts, back, sums, arrived, share, taken,
    load_sem, halo_send, halo_recv, mark_send, mark_recv, z_send, z_recv, a_send, a_recv,
    b_send, b_recv, w_send, w_recv, r_send, r_recv, g_send, g_recv,
):
    me, row = lax.axis_index("exp"), lax.axis_index("rep")
    tok, feature = tokens.shape
    units = w_up.shape[1]
    tiles = ranks // PAIR
    buddy = row + 1 - 2 * lax.rem(row, 2)
    head_size = feature // HEADS

    def partner(j):
        return lax.rem(row + PAIR * j, ranks)

    loads = [
        pltpu.make_async_copy(source, target, load_sem.at[i])
        for i, (source, target) in enumerate(
            ((w_up_hbm, w_up.at[0]), (w_down_hbm, w_down.at[0]), (w_qkv_hbm, w_qkv), (w_proj_hbm, w_proj))
        )
    ]
    for load in loads:
        load.start()

    barrier = pltpu.get_barrier_semaphore()

    def near(v, h):
        conds = []
        if v:
            conds.append((row + v >= 0) & (row + v < ranks))
        if h:
            conds.append((me + h >= 0) & (me + h < ring))
        return conds[0] if len(conds) == 1 else conds[0] & conds[1]

    def greet_ring(step, carry):
        pl.semaphore_signal(barrier, device_id={"exp": lax.rem(me + step, ring)})
        return carry

    def greet_ranks(step, carry):
        pl.semaphore_signal(barrier, device_id={"rep": lax.rem(row + step, ranks)})
        return carry

    lax.fori_loop(1, ring, greet_ring, 0)
    lax.fori_loop(1, ranks, greet_ranks, 0)
    for v, h in SIDES:
        if v and h:
            @pl.when(near(v, h))
            def _():
                pl.semaphore_signal(barrier, device_id={"rep": row + v, "exp": me + h})

    spots = wins.spots(tile_cols, tok)
    perm = (lax.broadcasted_iota(jnp.int32, (tok, tok), 0) == spots).astype(f32).astype(bf16)
    grouped[...] = dot(perm, tokens[...]).astype(bf16)
    for number, (i, j, start, sizes) in enumerate(wins.wins):
        ext[pl.ds(number * wins.cells, sizes[0]), :] = grouped[pl.ds(start, sizes[0]), :]
    for v, h in SIDES:
        @pl.when(jnp.logical_not(near(v, h)))
        def _():
            for _, place, rows in wins.pieces(v, h):
                ext[pl.ds(place, rows), :] = jnp.zeros((rows, feature), bf16)

    down = (row + ranks - 1) // ranks + (2 * ranks - 2 - row) // ranks
    across = (me + ring - 1) // ring + (2 * ring - 2 - me) // ring
    pl.semaphore_wait(barrier, ring - 1 + ranks - 1 + down * across)

    for index, (v, h) in enumerate(SIDES):
        @pl.when(near(v, h))
        def _():
            device = {"rep": row + v} if not h else {"exp": me + h} if not v else {"rep": row + v, "exp": me + h}
            for source, place, rows in wins.pieces(-v, -h):
                pltpu.make_async_remote_copy(
                    src_ref=grouped.at[pl.ds(source, rows)],
                    dst_ref=ext.at[pl.ds(place, rows)],
                    send_sem=halo_send.at[index],
                    recv_sem=halo_recv.at[len(SIDES) - 1 - index],
                    device_id=device,
                ).start()

    lanes = max(8, ring)
    routes = route[0:1, :].astype(f32)
    match = (lax.broadcasted_iota(jnp.int32, (lanes, tok), 0).astype(f32) == routes).astype(f32)
    before = (
        lax.broadcasted_iota(jnp.int32, (tok, tok), 0) < lax.broadcasted_iota(jnp.int32, (tok, tok), 1)
    ).astype(f32).astype(bf16)
    earlier = dot(match.astype(bf16), before)
    ids = routes * cap + jnp.sum(match * earlier, axis=0, keepdims=True)
    marks[0] = jnp.broadcast_to(ids.astype(jnp.int32), marks.shape[1:])

    def send_marks(j):
        pltpu.make_async_remote_copy(
            src_ref=marks.at[0],
            dst_ref=marks.at[tiles - j],
            send_sem=mark_send.at[j],
            recv_sem=mark_recv.at[tiles - j],
            device_id={"rep": partner(j)},
        ).start()

    def send_tokens(t, source, j):
        pltpu.make_async_remote_copy(
            src_ref=source,
            dst_ref=held.at[t, tiles - j],
            send_sem=z_send.at[t, j],
            recv_sem=z_recv.at[t, tiles - j],
            device_id={"rep": partner(j)},
        ).start()

    def make_placer(j):
        slot_ids = lax.broadcasted_iota(jnp.int32, placers.shape[1:], 0)
        placers[j] = (slot_ids == marks[j, 0:1, :]).astype(f32).astype(bf16)

    def swap(source, target, send_sem, recv_sem):
        mine = pl.ds(pl.multiple_of(me * cap, 16), cap)

        def send(step, carry):
            peer = lax.rem(me + step, ring)
            pltpu.make_async_remote_copy(
                src_ref=source.at[pl.ds(pl.multiple_of(peer * cap, 16), cap)],
                dst_ref=target.at[mine],
                send_sem=send_sem,
                recv_sem=recv_sem,
                device_id={"exp": peer},
            ).start()
            return carry

        lax.fori_loop(1, ring, send, 0)
        pltpu.make_async_copy(source.at[mine], target.at[mine], recv_sem).start()

    def dispatch(t, j, values):
        slots[t, j] = dot(placers[j], values).astype(bf16)
        swap(slots.at[t, j], gathered.at[t, j], a_send.at[t, j], a_recv.at[t, j])

    each(1, tiles, send_marks)
    grid_row = lax.broadcasted_iota(jnp.int32, (tok, gate.shape[0]), 0) // tile_cols
    picks = (grid_row == lax.broadcasted_iota(jnp.int32, (tok, gate.shape[0]), 1)).astype(f32)
    gate_rows = lax.dot_general(
        picks, gate[...], (((1,), (0,)), ((), ())), precision=lax.Precision.HIGHEST, preferred_element_type=f32
    )
    grid_col = lax.rem(lax.broadcasted_iota(jnp.int32, (tok, tile_cols), 0), tile_cols)
    chosen = jnp.where(grid_col == lax.broadcasted_iota(jnp.int32, (tok, tile_cols), 1), gate_rows, 0.0)
    gate_col[...] = jnp.broadcast_to(jnp.sum(chosen, axis=1, keepdims=True), gate_col.shape)
    upstream[...] = (gate_col[:, 0:1] * cotangent[...].astype(f32)).astype(bf16)
    each(1, tiles, lambda j: send_tokens(0, upstream, j))
    make_placer(0)
    dispatch(0, 0, upstream[...])

    def send_weight(index, weight):
        loads[index].wait()
        pltpu.make_async_remote_copy(
            src_ref=weight.at[0],
            dst_ref=weight.at[1],
            send_sem=w_send.at[index],
            recv_sem=w_recv.at[index],
            device_id={"rep": buddy},
        ).start()

    send_weight(0, w_up)

    loads[2].wait()
    queries[...] = dot(grouped[...], w_qkv[:, :feature]).astype(bf16)
    for index, (v, h) in enumerate(SIDES):
        @pl.when(near(v, h))
        def _():
            amount = sum(rows for _, _, rows in wins.pieces(v, h))
            drain(grouped.at[pl.ds(0, amount)], halo_recv.at[index])

    kv[...] = dot(ext[...], w_qkv[:, feature:]).astype(bf16)
    key_lane = lax.broadcasted_iota(jnp.int32, (1, wins.cells), 1)
    group = 128 // head_size

    def attend(number):
        i, j, start, sizes = wins.wins[number]
        amount = sizes[0]
        absent = jnp.zeros((1, wins.cells), f32)
        v = -1 if i == 0 else 1 if i == wins.last[0] else 0
        h = -1 if j == 0 else 1 if j == wins.last[1] else 0
        for side in {(v, 0), (0, h), (v, h)} - {(0, 0)}:
            kind = (1 if side[0] else 0) + (2 if side[1] else 0)
            first = sum(sizes[:kind])
            inside = (key_lane >= first) & (key_lane < first + sizes[kind])
            missing = jnp.where(near(*side), 0.0, -1e30)
            absent = jnp.where(inside, missing, absent)
        lane = lax.broadcasted_iota(jnp.int32, (amount, 128), 1)
        keep = [((lane >= g * head_size) & (lane < (g + 1) * head_size)).astype(f32) for g in range(group)]
        mine, theirs = pl.ds(start, amount), pl.ds(number * wins.cells, wins.cells)
        for first in range(0, feature, 128):
            query = queries[mine, pl.ds(first, 128)]
            stacked = jnp.concatenate([query * k.astype(bf16) for k in keep], axis=0)
            scores = dot_t(stacked, kv[theirs, pl.ds(first, 128)]) * (1.0 / math.sqrt(head_size)) + absent
            weights = jnp.exp(scores - jnp.max(scores, axis=-1, keepdims=True))
            total = jnp.sum(weights, axis=-1, keepdims=True)
            probs = (weights * (1.0 / total)).astype(bf16)
            found = dot(probs, kv[theirs, pl.ds(feature + first, 128)])
            picked = sum(k * found[g * amount : (g + 1) * amount] for g, k in enumerate(keep))
            context[mine, pl.ds(first, 128)] = picked.astype(bf16)

    def bring(t, j):
        if t == 0:
            drain(marks.at[0], mark_recv.at[j])
            make_placer(j)
        drain(held.at[t, j], z_recv.at[t, j])
        dispatch(t, j, held[t, j])

    for number in range(len(wins.wins)):
        attend(number)

    loads[3].wait()
    attended = dot(context[...], w_proj[...])
    blended = (grouped[...].astype(f32) + layer_norm(attended)).astype(bf16)
    mixed[...] = t_dot(perm, blended).astype(bf16)
    each(1, tiles, lambda j: send_tokens(1, mixed, j))
    dispatch(1, 0, mixed[...])
    send_weight(1, w_down)
    each(1, tiles, lambda j: bring(0, j))

    block = min(256, units)

    def arrive(j):
        for t in range(2):
            drain(gathered.at[t, j], a_recv.at[t, j])

    def stage(j, half):
        for first in range(0, units, block):
            spot = pl.ds(half * units + first, block)
            pre = dot_t(gathered[1, j], w_up[half, pl.ds(first, block), :])
            flow = dot_t(gathered[0, j], w_down[half, pl.ds(first, block), :])
            square = pre * pre
            inner = jnp.tanh(GELU_C * (pre + 0.044715 * square * pre))
            hidden[j, :, spot] = (0.5 * pre * (1.0 + inner)).astype(bf16)
            slope = 0.5 * (1.0 + inner) + 0.5 * pre * (1.0 - inner * inner) * GELU_C * (
                1.0 + 3.0 * 0.044715 * square
            )
            pre_grad[j, :, spot] = (flow * slope).astype(bf16)

    def outputs(j):
        for t, (left, right) in enumerate(((hidden, w_down), (pre_grad, w_up))):
            total = dot(left[j, :, pl.ds(0, units)], right[0])
            for half in range(1, PAIR):
                total += dot(left[j, :, pl.ds(half * units, units)], right[half])
            parts[t, j] = total.astype(bf16)
            swap(parts.at[t, j], back.at[t, j], b_send.at[t, j], b_recv.at[t, j])

    def near_half(j):
        arrive(j)
        stage(j, 0)

    near_half(0)
    each(1, tiles, lambda j: bring(1, j))
    each(1, tiles, near_half)
    for index, weight in enumerate((w_up, w_down)):
        drain(weight.at[1], w_recv.at[index])
    each(1, tiles, lambda j: stage(j, 1))
    each(1, tiles, outputs)
    stage(0, 1)

    rows = tiles * hidden.shape[1]

    def gradient(t, half):
        left = (pre_grad, hidden)[t][...].reshape(rows, PAIR * units)[:, half * units : (half + 1) * units]
        return t_dot(left, gathered[1 - t].reshape(rows, feature))

    for t in range(2):
        share[t] = gradient(t, 1).astype(bf16)
        pltpu.make_async_remote_copy(
            src_ref=share.at[t],
            dst_ref=taken.at[t],
            send_sem=g_send.at[t],
            recv_sem=g_recv.at[t],
            device_id={"rep": buddy},
        ).start()

    outputs(0)

    def placed(t, j):
        drain(back.at[t, j], b_recv.at[t, j])
        return t_dot(placers[j], back[t, j])

    def give(j):
        for t in range(2):
            sums[t, j] = placed(t, j).astype(bf16)
            pltpu.make_async_remote_copy(
                src_ref=sums.at[t, j],
                dst_ref=arrived.at[t, tiles - j],
                send_sem=r_send.at[t, j],
                recv_sem=r_recv.at[t, tiles - j],
                device_id={"rep": partner(j)},
            ).start()

    each(1, tiles, give)
    grad_up[...] = gradient(0, 0)
    grad_down[...] = gradient(1, 0)

    def total_of(t):
        value = placed(t, 0)
        for j in range(1, tiles):
            drain(arrived.at[t, j], r_recv.at[t, j])
            value += arrived[t, j].astype(f32)
        return value

    layer_out[...] = (mixed[...].astype(f32) + gate_col[:, 0:1] * total_of(0)).astype(bf16)
    input_grad[...] = total_of(1).astype(bf16)
    factor = 1.0 / ranks
    for t, out in enumerate((grad_up, grad_down)):
        drain(taken.at[t], g_recv.at[t])
        out[...] = (out[...] + taken[t].astype(f32)) * factor

    for index, (v, h) in enumerate(SIDES):
        @pl.when(near(v, h))
        def _():
            amount = sum(rows for _, _, rows in wins.pieces(-v, -h))
            drain(grouped.at[pl.ds(0, amount)], halo_send.at[index])

    for t in range(2):
        drain(w_up.at[0], w_send.at[t])
        drain(share.at[t], g_send.at[t])

    def finish(j):
        for t in range(2):
            sent = slots.at[t, j, pl.ds(0, (ring - 1) * cap)]
            drain(sent, a_send.at[t, j])
            drain(sent, b_send.at[t, j])

    each(0, tiles, finish)

    def finish_far(j):
        drain(marks.at[0], mark_send.at[j])
        for t in range(2):
            drain(mixed, z_send.at[t, j])
            drain(mixed, r_send.at[t, j])

    each(1, tiles, finish_far)


def store(*values):
    count = len(values)

    def body(*refs):
        sems = refs[2 * count]
        copies = [pltpu.make_async_copy(refs[i], refs[count + i], sems.at[i]) for i in range(count)]
        for copy in copies:
            copy.start()
        for copy in copies:
            copy.wait()

    return pl.pallas_call(
        body,
        name="store",
        out_shape=tuple(jax.ShapeDtypeStruct(v.shape, v.dtype) for v in values),
        in_specs=[pl.BlockSpec(memory_space=pltpu.VMEM)] * count,
        out_specs=(pl.BlockSpec(memory_space=pl.ANY),) * count,
        scratch_shapes=[pltpu.SemaphoreType.DMA((count,))],
        compiler_params=pltpu.CompilerParams(vmem_limit_bytes=8 << 20),
    )(*values)


def per_device(ranks, ring, tokens, gate, route, cotangent, w_qkv, w_proj, w_up, w_down):
    tile_rows, tile_cols, feature = tokens.shape
    tok = tile_rows * tile_cols
    units = w_up.shape[1]
    capacity = max(2, 3 * tok // (2 * ring))
    capacity = -(-capacity // 16) * 16
    rows = ring * capacity
    tiles = ranks // PAIR
    wins = Windows(tile_rows, tile_cols)
    ext = len(wins.wins) * wins.cells

    def body(*refs):
        layer_kernel(wins, ring, ranks, capacity, tile_cols, *refs)

    vmem, hbm = pl.BlockSpec(memory_space=pltpu.VMEM), pl.BlockSpec(memory_space=pltpu.HBM)
    dma = pltpu.SemaphoreType.DMA
    buffers = [
        pltpu.VMEM(w_qkv.shape, bf16),
        pltpu.VMEM(w_proj.shape, bf16),
        pltpu.VMEM((PAIR, units, feature), bf16),
        pltpu.VMEM((PAIR, units, feature), bf16),
        pltpu.VMEM((tok, feature), bf16),
        pltpu.VMEM((ext, feature), bf16),
        pltpu.VMEM((ext, 2 * feature), bf16),
        pltpu.VMEM((tok, feature), bf16),
        pltpu.VMEM((tok, feature), bf16),
        pltpu.VMEM((tok, feature), bf16),
        pltpu.VMEM((tok, feature), bf16),
        pltpu.VMEM((tok, 128), f32),
        pltpu.VMEM((tiles, 8, tok), jnp.int32),
        pltpu.VMEM((tiles, rows, tok), bf16),
        pltpu.VMEM((2, tiles, tok, feature), bf16),
        pltpu.VMEM((2, tiles, rows, feature), bf16),
        pltpu.VMEM((2, tiles, rows, feature), bf16),
        pltpu.VMEM((tiles, rows, PAIR * units), bf16),
        pltpu.VMEM((tiles, rows, PAIR * units), bf16),
        pltpu.VMEM((2, tiles, rows, feature), bf16),
        pltpu.VMEM((2, tiles, rows, feature), bf16),
        pltpu.VMEM((2, tiles, tok, feature), bf16),
        pltpu.VMEM((2, tiles, tok, feature), bf16),
        pltpu.VMEM((2, units, feature), bf16),
        pltpu.VMEM((2, units, feature), bf16),
    ]
    semaphores = [
        dma((4,)),
        dma((len(SIDES),)),
        dma((len(SIDES),)),
        dma((tiles,)),
        dma((tiles,)),
        dma((2, tiles)),
        dma((2, tiles)),
        dma((2, tiles)),
        dma((2, tiles)),
        dma((2, tiles)),
        dma((2, tiles)),
        dma((2,)),
        dma((2,)),
        dma((2, tiles)),
        dma((2, tiles)),
        dma((2,)),
        dma((2,)),
    ]
    held_bytes = sum(math.prod(ref.shape) * jnp.dtype(ref.dtype).itemsize for ref in buffers)
    limit = min(60 << 20, held_bytes + (16 << 20))
    layer_out, input_grad, grad_up, grad_down = pl.pallas_call(
        body,
        name="layer",
        out_shape=(
            jax.ShapeDtypeStruct((tok, feature), bf16),
            jax.ShapeDtypeStruct((tok, feature), bf16),
            jax.ShapeDtypeStruct((units, feature), f32),
            jax.ShapeDtypeStruct((units, feature), f32),
        ),
        in_specs=[vmem] * 4 + [hbm] * 4,
        out_specs=(vmem,) * 4,
        scratch_shapes=buffers + semaphores,
        compiler_params=pltpu.CompilerParams(
            collective_id=0, has_side_effects=True, vmem_limit_bytes=limit
        ),
    )(
        *(
            pltpu.with_memory_space_constraint(array, pltpu.HBM)
            for array in (
                tokens.reshape(tok, feature),
                cotangent.reshape(tok, feature),
                gate,
                route.reshape(1, tok),
                w_qkv,
                w_proj,
                w_up[0],
                w_down[0],
            )
        )
    )
    layer_out, input_grad, grad_up, grad_down = store(layer_out, input_grad, grad_up, grad_down)
    return (
        layer_out.reshape(tile_rows, tile_cols, feature),
        input_grad.reshape(tile_rows, tile_cols, feature),
        grad_up[None],
        grad_down[None],
    )


def solution(mesh):
    ranks, ring = mesh.shape["rep"], mesh.shape["exp"]
    placed = (
        P("rep", "exp", None),
        P("rep", "exp"),
        P("rep", "exp", None, None),
        P("rep", "exp", None),
        P(),
        P(),
        P("exp", "rep", None),
        P("exp", "rep", None),
    )

    def device(*arrays):
        return per_device(ranks, ring, *arrays)

    return jax.shard_map(
        device,
        mesh=mesh,
        in_specs=placed,
        out_specs=(
            P("rep", "exp", None),
            P("rep", "exp", None),
            P("exp", "rep", None),
            P("exp", "rep", None),
        ),
        check_vma=False,
    )
```

```python
import math

import jax
import jax.numpy as jnp
import numpy as np
from jax import lax
from jax.experimental import pallas as pl
from jax.experimental.pallas import tpu as pltpu
from jax.sharding import PartitionSpec as P

HEADS = 16
GELU_C = math.sqrt(2.0 / math.pi)
window_side = 8
margin_cells = 4
WEIGHT_PARTS, AHEAD, EARLY_G, NEARER = 2, 1, True, False
PAIR = 2
f32, bf16 = jnp.float32, jnp.bfloat16


class Windows:
    def __init__(self, tile_rows, tile_cols):
        def cut(size):
            parts = [margin_cells] + [window_side] * ((size - 2 * margin_cells) // window_side)
            return parts + [margin_cells]

        self.heights, self.widths = cut(tile_rows), cut(tile_cols)
        self.cells = window_side * window_side
        self.wins, start = [], 0
        for i, h in enumerate(self.heights):
            for j, w in enumerate(self.widths):
                sizes = (h * w, (window_side - h) * w, h * (window_side - w), (window_side - h) * (window_side - w))
                self.wins.append((i, j, start, sizes))
                start += h * w
        self.last = (len(self.heights) - 1, len(self.widths) - 1)

    def spots(self, tile_cols, tok):
        lane = lax.broadcasted_iota(jnp.int32, (1, tok), 1)
        rows, cols = lane // tile_cols, lax.rem(lane, tile_cols)

        def within(line, sizes):
            first, size, top = jnp.zeros_like(line), jnp.full_like(line, sizes[0]), 0
            for before, here in zip(sizes, sizes[1:]):
                top += before
                first, size = jnp.where(line >= top, top, first), jnp.where(line >= top, here, size)
            return first, size

        (top, height), (left, width) = within(rows, self.heights), within(cols, self.widths)
        return top * tile_cols + left * height + (rows - top) * width + cols - left

    def number(self, i, j):
        return i * len(self.widths) + j

    def segment(self, number, kind):
        sizes = self.wins[number][3]
        return number * self.cells + sum(sizes[:kind]), sizes[kind]

    def pieces(self, dv, dh):
        found = []
        for number, (i, j, _, _) in enumerate(self.wins):
            vertical = (dv == -1 and i == 0) or (dv == 1 and i == self.last[0])
            beside = (dh == -1 and j == 0) or (dh == 1 and j == self.last[1])
            if (dv and not vertical) or (dh and not beside):
                continue
            kind = (1 if dv else 0) + (2 if dh else 0)
            theirs = self.number(self.last[0] - i if dv else i, self.last[1] - j if dh else j)
            place, rows = self.segment(number, kind)
            found.append((self.wins[theirs][2], place, rows))
        return found


class Plan:
    def __init__(self, ranks, nearer):
        def handler(tile, pair):
            low = PAIR * pair
            if tile // PAIR == pair:
                return tile
            return (low if tile < low else low + 1) if nearer else low + tile % PAIR

        handled = [[t for t in range(ranks) if handler(t, p // PAIR) == p] for p in range(ranks)]
        self.tiles = [sorted(own, key=lambda t, p=p: (abs(t - p), t)) for p, own in enumerate(handled)]
        self.far = [[p for p in range(ranks) if p != t and t in self.tiles[p]] for t in range(ranks)]
        self.most = max(len(own) for own in self.tiles)
        self.sends = max(len(to) for to in self.far)
        self.counts = sorted({len(own) for own in self.tiles})
        assert len({len(to) for to in self.far}) == 1

    @staticmethod
    def pick(row, values):
        value = values[-1]
        if len(set(values)) > 1:
            for rank, other in enumerate(values[:-1]):
                value = jnp.where(row == rank, other, value)
        return value

    def handles(self, row, j):
        flags = [len(own) > j for own in self.tiles]
        return True if all(flags) else self.pick(row, [int(f) for f in flags]) == 1

    def has(self, row, count):
        return True if len(self.counts) == 1 else self.pick(row, [len(own) for own in self.tiles]) == count

    def origin(self, row, j):
        known = [(own[j], self.far[own[j]].index(p)) if len(own) > j else (0, 0) for p, own in enumerate(self.tiles)]
        return self.pick(row, [t for t, _ in known]), self.pick(row, [k for _, k in known])

    def goal(self, row, k):
        return (
            self.pick(row, [to[k] for to in self.far]),
            self.pick(row, [self.tiles[to[k]].index(t) for t, to in enumerate(self.far)]),
        )


def when(condition, body):
    if condition is True:
        body()
    else:
        pl.when(condition)(body)


SIDES = [(v, h) for v in (-1, 0, 1) for h in (-1, 0, 1) if (v, h) != (0, 0)]


def drain(ref, sem):
    pltpu.make_async_copy(ref, ref, sem).wait()


def dot_t(a, b):
    return lax.dot_general(a, b, (((1,), (1,)), ((), ())), preferred_element_type=f32)


def t_dot(a, b):
    return lax.dot_general(a, b, (((0,), (0,)), ((), ())), preferred_element_type=f32)


def dot(a, b):
    return jnp.dot(a, b, preferred_element_type=f32)


def layer_norm(values):
    average = jnp.mean(values, axis=-1, keepdims=True)
    centred = values - average
    spread = jnp.mean(centred * centred, axis=-1, keepdims=True)
    return centred * lax.rsqrt(spread + 1e-05)


def layer_kernel(
    wins, plan, ring, ranks, cap, tile_cols,
    tokens_hbm, cotangent_hbm, gate_hbm, route_hbm, w_qkv_hbm, w_proj_hbm, w_up_hbm, w_down_hbm,
    layer_out, input_grad, grad_up, grad_down,
    tokens, cotangent, gate, route, w_qkv, w_proj, w_up, w_down, grouped, ext, kv, queries, context, mixed, upstream, gate_col,
    marks, placers, held, slots, gathered, hidden, slopes, pre_grad, parts, back, sums, arrived, share, taken,
    load_sem, halo_send, halo_recv, mark_send, mark_recv, z_send, z_recv, a_send, a_recv,
    b_send, b_recv, w_send, w_recv, r_send, r_recv, g_send, g_recv,
):
    me, row = lax.axis_index("exp"), lax.axis_index("rep")
    tok, feature = tokens.shape
    units = w_up.shape[1]
    tiles, sends = plan.most, plan.sends
    buddy = row + 1 - 2 * lax.rem(row, 2)
    head_size = feature // HEADS

    def others(body):
        for j in range(1, tiles):
            when(plan.handles(row, j), lambda j=j: body(j))

    loads = {
        name: pltpu.make_async_copy(source, target, load_sem.at[i])
        for i, (name, source, target) in enumerate(
            (
                ("tokens", tokens_hbm, tokens),
                ("route", route_hbm, route),
                ("gate", gate_hbm, gate),
                ("cotangent", cotangent_hbm, cotangent),
                ("up", w_up_hbm, w_up.at[0]),
                ("qkv", w_qkv_hbm, w_qkv),
                ("down", w_down_hbm, w_down.at[0]),
                ("proj", w_proj_hbm, w_proj),
            )
        )
    }
    for load in loads.values():
        load.start()

    barrier = pltpu.get_barrier_semaphore()

    def near(v, h):
        conds = []
        if v:
            conds.append((row + v >= 0) & (row + v < ranks))
        if h:
            conds.append((me + h >= 0) & (me + h < ring))
        return conds[0] if len(conds) == 1 else conds[0] & conds[1]

    def greet_ring(step, carry):
        pl.semaphore_signal(barrier, device_id={"exp": lax.rem(me + step, ring)})
        return carry

    def greet_ranks(step, carry):
        pl.semaphore_signal(barrier, device_id={"rep": lax.rem(row + step, ranks)})
        return carry

    lax.fori_loop(1, ring, greet_ring, 0)
    lax.fori_loop(1, ranks, greet_ranks, 0)
    for v, h in SIDES:
        if v and h:
            @pl.when(near(v, h))
            def _():
                pl.semaphore_signal(barrier, device_id={"rep": row + v, "exp": me + h})

    spots = wins.spots(tile_cols, tok)
    perm = (lax.broadcasted_iota(jnp.int32, (tok, tok), 0) == spots).astype(f32).astype(bf16)
    loads["tokens"].wait()
    grouped[...] = dot(perm, tokens[...]).astype(bf16)
    for number, (i, j, start, sizes) in enumerate(wins.wins):
        ext[pl.ds(number * wins.cells, sizes[0]), :] = grouped[pl.ds(start, sizes[0]), :]
    for v, h in SIDES:
        @pl.when(jnp.logical_not(near(v, h)))
        def _():
            for _, place, rows in wins.pieces(v, h):
                ext[pl.ds(place, rows), :] = jnp.zeros((rows, feature), bf16)

    down = (row + ranks - 1) // ranks + (2 * ranks - 2 - row) // ranks
    across = (me + ring - 1) // ring + (2 * ring - 2 - me) // ring
    pl.semaphore_wait(barrier, ring - 1 + ranks - 1 + down * across)

    for index, (v, h) in enumerate(SIDES):
        @pl.when(near(v, h))
        def _():
            device = {"rep": row + v} if not h else {"exp": me + h} if not v else {"rep": row + v, "exp": me + h}
            for source, place, rows in wins.pieces(-v, -h):
                pltpu.make_async_remote_copy(
                    src_ref=grouped.at[pl.ds(source, rows)],
                    dst_ref=ext.at[pl.ds(place, rows)],
                    send_sem=halo_send.at[index],
                    recv_sem=halo_recv.at[len(SIDES) - 1 - index],
                    device_id=device,
                ).start()

    lanes = max(8, ring)
    loads["route"].wait()
    routes = route[0:1, :].astype(f32)
    match = (lax.broadcasted_iota(jnp.int32, (lanes, tok), 0).astype(f32) == routes).astype(f32)
    before = (
        lax.broadcasted_iota(jnp.int32, (tok, tok), 0) < lax.broadcasted_iota(jnp.int32, (tok, tok), 1)
    ).astype(f32).astype(bf16)
    earlier = dot(match.astype(bf16), before)
    ids = routes * cap + jnp.sum(match * earlier, axis=0, keepdims=True)
    marks[0] = jnp.broadcast_to(ids.astype(jnp.int32), marks.shape[1:])

    def send_marks():
        for k in range(sends):
            goal, place = plan.goal(row, k)
            pltpu.make_async_remote_copy(
                src_ref=marks.at[0],
                dst_ref=marks.at[place],
                send_sem=mark_send.at[k],
                recv_sem=mark_recv.at[place],
                device_id={"rep": goal},
            ).start()

    def send_tokens(t, source):
        for k in range(sends):
            goal, place = plan.goal(row, k)
            pltpu.make_async_remote_copy(
                src_ref=source,
                dst_ref=held.at[t, place],
                send_sem=z_send.at[t, k],
                recv_sem=z_recv.at[t, place],
                device_id={"rep": goal},
            ).start()

    def make_placer(j):
        slot_ids = lax.broadcasted_iota(jnp.int32, placers.shape[1:], 0)
        placers[j] = (slot_ids == marks[j, 0:1, :]).astype(f32).astype(bf16)

    def swap(source, target, send_sem, recv_sem):
        mine = pl.ds(pl.multiple_of(me * cap, 16), cap)

        def send(step, carry):
            peer = lax.rem(me + step, ring)
            pltpu.make_async_remote_copy(
                src_ref=source.at[pl.ds(pl.multiple_of(peer * cap, 16), cap)],
                dst_ref=target.at[mine],
                send_sem=send_sem,
                recv_sem=recv_sem,
                device_id={"exp": peer},
            ).start()
            return carry

        lax.fori_loop(1, ring, send, 0)
        pltpu.make_async_copy(source.at[mine], target.at[mine], recv_sem).start()

    def dispatch(t, j, values):
        slots[t, j] = dot(placers[j], values).astype(bf16)
        swap(slots.at[t, j], gathered.at[t, j], a_send.at[t, j], a_recv.at[t, j])


    def wait_halo():
        for index, (v, h) in enumerate(SIDES):
            @pl.when(near(v, h))
            def _():
                amount = sum(rows for _, _, rows in wins.pieces(v, h))
                drain(grouped.at[pl.ds(0, amount)], halo_recv.at[index])

    loads["gate"].wait()
    loads["cotangent"].wait()
    grid_row = lax.broadcasted_iota(jnp.int32, (tok, gate.shape[0]), 0) // tile_cols
    picks = (grid_row == lax.broadcasted_iota(jnp.int32, (tok, gate.shape[0]), 1)).astype(f32)
    gate_rows = lax.dot_general(
        picks, gate[...], (((1,), (0,)), ((), ())), precision=lax.Precision.HIGHEST, preferred_element_type=f32
    )
    grid_col = lax.rem(lax.broadcasted_iota(jnp.int32, (tok, tile_cols), 0), tile_cols)
    chosen = jnp.where(grid_col == lax.broadcasted_iota(jnp.int32, (tok, tile_cols), 1), gate_rows, 0.0)
    gate_col[...] = jnp.broadcast_to(jnp.sum(chosen, axis=1, keepdims=True), gate_col.shape)
    upstream[...] = (gate_col[:, 0:1] * cotangent[...].astype(f32)).astype(bf16)
    make_placer(0)

    loads["qkv"].wait()
    queries[...] = dot(grouped[...], w_qkv[:, :feature]).astype(bf16)
    if not EARLY_G:
        wait_halo()
    send_marks()
    send_tokens(0, upstream)
    dispatch(0, 0, upstream[...])

    chunk = units // WEIGHT_PARTS
    weights = [(m, p) for m in range(2) for p in range(WEIGHT_PARTS)]

    def weight_part(half, number):
        m, p = weights[number]
        return (w_up, w_down)[m].at[half, pl.ds(p * chunk, chunk)]

    def send_weights(numbers):
        for number in numbers:
            pltpu.make_async_remote_copy(
                src_ref=weight_part(0, number),
                dst_ref=weight_part(1, number),
                send_sem=w_send.at[number],
                recv_sem=w_recv.at[number],
                device_id={"rep": buddy},
            ).start()

    loads["up"].wait()
    loads["down"].wait()
    send_weights(range(AHEAD))
    if EARLY_G:
        wait_halo()
    kv[...] = dot(ext[...], w_qkv[:, feature:]).astype(bf16)
    key_lane = lax.broadcasted_iota(jnp.int32, (1, wins.cells), 1)
    group = 128 // head_size

    def attend(number):
        i, j, start, sizes = wins.wins[number]
        amount = sizes[0]
        absent = jnp.zeros((1, wins.cells), f32)
        v = -1 if i == 0 else 1 if i == wins.last[0] else 0
        h = -1 if j == 0 else 1 if j == wins.last[1] else 0
        for side in {(v, 0), (0, h), (v, h)} - {(0, 0)}:
            kind = (1 if side[0] else 0) + (2 if side[1] else 0)
            first = sum(sizes[:kind])
            inside = (key_lane >= first) & (key_lane < first + sizes[kind])
            missing = jnp.where(near(*side), 0.0, -1e30)
            absent = jnp.where(inside, missing, absent)
        lane = lax.broadcasted_iota(jnp.int32, (amount, 128), 1)
        keep = [((lane >= g * head_size) & (lane < (g + 1) * head_size)).astype(f32) for g in range(group)]
        mine, theirs = pl.ds(start, amount), pl.ds(number * wins.cells, wins.cells)
        for first in range(0, feature, 128):
            query = queries[mine, pl.ds(first, 128)]
            stacked = jnp.concatenate([query * k.astype(bf16) for k in keep], axis=0)
            scores = dot_t(stacked, kv[theirs, pl.ds(first, 128)]) * (1.0 / math.sqrt(head_size)) + absent
            weights = jnp.exp(scores - jnp.max(scores, axis=-1, keepdims=True))
            total = jnp.sum(weights, axis=-1, keepdims=True)
            probs = (weights * (1.0 / total)).astype(bf16)
            found = dot(probs, kv[theirs, pl.ds(feature + first, 128)])
            picked = sum(k * found[g * amount : (g + 1) * amount] for g, k in enumerate(keep))
            context[mine, pl.ds(first, 128)] = picked.astype(bf16)

    def bring(t, j):
        if t == 0:
            drain(marks.at[0], mark_recv.at[j])
            make_placer(j)
        drain(held.at[t, j], z_recv.at[t, j])
        dispatch(t, j, held[t, j])

    for number in range(len(wins.wins)):
        attend(number)

    loads["proj"].wait()
    attended = dot(context[...], w_proj[...])
    blended = (grouped[...].astype(f32) + layer_norm(attended)).astype(bf16)
    mixed[...] = t_dot(perm, blended).astype(bf16)
    send_tokens(1, mixed)
    dispatch(1, 0, mixed[...])
    send_weights(range(AHEAD, len(weights)))
    others(lambda j: bring(0, j))

    block = min(256, units)

    def arrive(j):
        for t in range(2):
            drain(gathered.at[t, j], a_recv.at[t, j])

    def rise(j, half):
        for first in range(0, units, block):
            pre = dot_t(gathered[1, j], w_up[half, pl.ds(first, block), :])
            square = pre * pre
            inner = jnp.tanh(GELU_C * (pre + 0.044715 * square * pre))
            hidden[j, :, pl.ds(half * units + first, block)] = (0.5 * pre * (1.0 + inner)).astype(bf16)
            slopes[j, :, pl.ds(first, block)] = 0.5 * (1.0 + inner) + 0.5 * pre * (1.0 - inner * inner) * GELU_C * (
                1.0 + 3.0 * 0.044715 * square
            )

    def fall(j, half):
        for first in range(0, units, block):
            flow = dot_t(gathered[0, j], w_down[half, pl.ds(first, block), :])
            spot = pl.ds(half * units + first, block)
            pre_grad[j, :, spot] = (flow * slopes[j, :, pl.ds(first, block)]).astype(bf16)

    def outputs(j):
        for t, (left, right) in enumerate(((hidden, w_down), (pre_grad, w_up))):
            total = dot(left[j, :, pl.ds(0, units)], right[0])
            for half in range(1, PAIR):
                total += dot(left[j, :, pl.ds(half * units, units)], right[half])
            parts[t, j] = total.astype(bf16)
            swap(parts.at[t, j], back.at[t, j], b_send.at[t, j], b_recv.at[t, j])

    def near_half(j):
        arrive(j)
        rise(j, 0)
        fall(j, 0)

    def gradient(t, half, count):
        left = (pre_grad, hidden)[t][0:count].reshape(count * hidden.shape[1], PAIR * units)
        right = gathered[1 - t, 0:count].reshape(count * hidden.shape[1], feature)
        return t_dot(left[:, half * units : (half + 1) * units], right)

    def give_gradient(t):
        for count in plan.counts:
            def partial(count=count):
                share[t] = gradient(t, 1, count).astype(bf16)

            when(plan.has(row, count), partial)
        pltpu.make_async_remote_copy(
            src_ref=share.at[t],
            dst_ref=taken.at[t],
            send_sem=g_send.at[t],
            recv_sem=g_recv.at[t],
            device_id={"rep": buddy},
        ).start()

    def await_weight(m):
        for number, (matrix, _) in enumerate(weights):
            if matrix == m:
                drain(weight_part(1, number), w_recv.at[number])

    near_half(0)
    others(lambda j: bring(1, j))
    others(near_half)
    await_weight(0)
    rise(0, 1)
    others(lambda j: rise(j, 1))
    give_gradient(1)
    await_weight(1)
    for j in range(tiles - 1, 0, -1):
        def far_tile(j=j):
            fall(j, 1)
            outputs(j)

        when(plan.handles(row, j), far_tile)
    fall(0, 1)
    give_gradient(0)
    outputs(0)

    def placed(t, j):
        drain(back.at[t, j], b_recv.at[t, j])
        return t_dot(placers[j], back[t, j])

    def give(j):
        goal, place = plan.origin(row, j)
        for t in range(2):
            sums[t, j] = placed(t, j).astype(bf16)
            pltpu.make_async_remote_copy(
                src_ref=sums.at[t, j],
                dst_ref=arrived.at[t, place],
                send_sem=r_send.at[t, j],
                recv_sem=r_recv.at[t, place],
                device_id={"rep": goal},
            ).start()

    for j in range(tiles - 1, 0, -1):
        when(plan.handles(row, j), lambda j=j: give(j))
    for count in plan.counts:
        def own_gradients(count=count):
            grad_up[...] = gradient(0, 0, count)
            grad_down[...] = gradient(1, 0, count)

        when(plan.has(row, count), own_gradients)

    def total_of(t):
        value = placed(t, 0)
        for k in range(sends):
            drain(arrived.at[t, k], r_recv.at[t, k])
            value += arrived[t, k].astype(f32)
        return value

    layer_out[...] = (mixed[...].astype(f32) + gate_col[:, 0:1] * total_of(0)).astype(bf16)
    input_grad[...] = total_of(1).astype(bf16)
    factor = 1.0 / ranks
    for t, out in enumerate((grad_up, grad_down)):
        drain(taken.at[t], g_recv.at[t])
        out[...] = (out[...] + taken[t].astype(f32)) * factor

    for index, (v, h) in enumerate(SIDES):
        @pl.when(near(v, h))
        def _():
            amount = sum(rows for _, _, rows in wins.pieces(-v, -h))
            drain(grouped.at[pl.ds(0, amount)], halo_send.at[index])

    for number in range(len(weights)):
        drain(weight_part(0, number), w_send.at[number])
    for t in range(2):
        drain(share.at[t], g_send.at[t])
        for k in range(sends):
            drain(mixed, z_send.at[t, k])
    for k in range(sends):
        drain(marks.at[0], mark_send.at[k])

    def finish(j):
        for t in range(2):
            sent = slots.at[t, j, pl.ds(0, (ring - 1) * cap)]
            drain(sent, a_send.at[t, j])
            drain(sent, b_send.at[t, j])
            if j:
                drain(mixed, r_send.at[t, j])

    finish(0)
    others(finish)


def store(*values):
    count = len(values)

    def body(*refs):
        sems = refs[2 * count]
        copies = [pltpu.make_async_copy(refs[i], refs[count + i], sems.at[i]) for i in range(count)]
        for copy in copies:
            copy.start()
        for copy in copies:
            copy.wait()

    return pl.pallas_call(
        body,
        name="store",
        out_shape=tuple(jax.ShapeDtypeStruct(v.shape, v.dtype) for v in values),
        in_specs=[pl.BlockSpec(memory_space=pltpu.VMEM)] * count,
        out_specs=(pl.BlockSpec(memory_space=pl.ANY),) * count,
        scratch_shapes=[pltpu.SemaphoreType.DMA((count,))],
        compiler_params=pltpu.CompilerParams(vmem_limit_bytes=8 << 20),
    )(*values)


def per_device(ranks, ring, tokens, gate, route, cotangent, w_qkv, w_proj, w_up, w_down):
    tile_rows, tile_cols, feature = tokens.shape
    tok = tile_rows * tile_cols
    units = w_up.shape[1]
    capacity = max(2, 3 * tok // (2 * ring))
    capacity = -(-capacity // 16) * 16
    rows = ring * capacity
    wins = Windows(tile_rows, tile_cols)
    ext = len(wins.wins) * wins.cells

    vmem, hbm = pl.BlockSpec(memory_space=pltpu.VMEM), pl.BlockSpec(memory_space=pltpu.HBM)
    dma = pltpu.SemaphoreType.DMA
    def buffers_of(plan):
        tiles, sends = plan.most, plan.sends
        return [
            pltpu.VMEM((tok, feature), bf16),
            pltpu.VMEM((tok, feature), bf16),
            pltpu.VMEM(gate.shape, f32),
            pltpu.VMEM((1, tok), jnp.int32),
            pltpu.VMEM(w_qkv.shape, bf16),
            pltpu.VMEM(w_proj.shape, bf16),
            pltpu.VMEM((PAIR, units, feature), bf16),
            pltpu.VMEM((PAIR, units, feature), bf16),
            pltpu.VMEM((tok, feature), bf16),
            pltpu.VMEM((ext, feature), bf16),
            pltpu.VMEM((ext, 2 * feature), bf16),
            pltpu.VMEM((tok, feature), bf16),
            pltpu.VMEM((tok, feature), bf16),
            pltpu.VMEM((tok, feature), bf16),
            pltpu.VMEM((tok, feature), bf16),
            pltpu.VMEM((tok, 128), f32),
            pltpu.VMEM((tiles, 8, tok), jnp.int32),
            pltpu.VMEM((tiles, rows, tok), bf16),
            pltpu.VMEM((2, tiles, tok, feature), bf16),
            pltpu.VMEM((2, tiles, rows, feature), bf16),
            pltpu.VMEM((2, tiles, rows, feature), bf16),
            pltpu.VMEM((tiles, rows, PAIR * units), bf16),
            pltpu.VMEM((tiles, rows, units), f32),
            pltpu.VMEM((tiles, rows, PAIR * units), bf16),
            pltpu.VMEM((2, tiles, rows, feature), bf16),
            pltpu.VMEM((2, tiles, rows, feature), bf16),
            pltpu.VMEM((2, tiles, tok, feature), bf16),
            pltpu.VMEM((2, max(1, sends), tok, feature), bf16),
            pltpu.VMEM((2, units, feature), bf16),
            pltpu.VMEM((2, units, feature), bf16),
        ]

    def size_of(plan):
        return sum(math.prod(ref.shape) * jnp.dtype(ref.dtype).itemsize for ref in buffers_of(plan))

    plan = Plan(ranks, NEARER)
    if size_of(plan) > 44 << 20:
        plan = Plan(ranks, False)
    buffers, limit = buffers_of(plan), min(63 << 20, size_of(plan) + (16 << 20))
    tiles, sends = plan.most, max(1, plan.sends)
    semaphores = [
        dma((8,)),
        dma((len(SIDES),)),
        dma((len(SIDES),)),
        dma((sends,)),
        dma((tiles,)),
        dma((2, sends)),
        dma((2, tiles)),
        dma((2, tiles)),
        dma((2, tiles)),
        dma((2, tiles)),
        dma((2, tiles)),
        dma((2 * WEIGHT_PARTS,)),
        dma((2 * WEIGHT_PARTS,)),
        dma((2, tiles)),
        dma((2, sends)),
        dma((2,)),
        dma((2,)),
    ]

    def body(*refs):
        layer_kernel(wins, plan, ring, ranks, capacity, tile_cols, *refs)

    layer_out, input_grad, grad_up, grad_down = pl.pallas_call(
        body,
        name="layer",
        out_shape=(
            jax.ShapeDtypeStruct((tok, feature), bf16),
            jax.ShapeDtypeStruct((tok, feature), bf16),
            jax.ShapeDtypeStruct((units, feature), f32),
            jax.ShapeDtypeStruct((units, feature), f32),
        ),
        in_specs=[hbm] * 8,
        out_specs=(vmem,) * 4,
        scratch_shapes=buffers + semaphores,
        compiler_params=pltpu.CompilerParams(
            collective_id=0, has_side_effects=True, vmem_limit_bytes=limit
        ),
    )(
        *(
            pltpu.with_memory_space_constraint(array, pltpu.HBM)
            for array in (
                tokens.reshape(tok, feature),
                cotangent.reshape(tok, feature),
                gate,
                route.reshape(1, tok),
                w_qkv,
                w_proj,
                w_up[0],
                w_down[0],
            )
        )
    )
    layer_out, input_grad, grad_up, grad_down = store(layer_out, input_grad, grad_up, grad_down)
    return (
        layer_out.reshape(tile_rows, tile_cols, feature),
        input_grad.reshape(tile_rows, tile_cols, feature),
        grad_up[None],
        grad_down[None],
    )


def solution(mesh):
    ranks, ring = mesh.shape["rep"], mesh.shape["exp"]
    placed = (
        P("rep", "exp", None),
        P("rep", "exp"),
        P("rep", "exp", None, None),
        P("rep", "exp", None),
        P(),
        P(),
        P("exp", "rep", None),
        P("exp", "rep", None),
    )

    def device(*arrays):
        return per_device(ranks, ring, *arrays)

    return jax.shard_map(
        device,
        mesh=mesh,
        in_specs=placed,
        out_specs=(
            P("rep", "exp", None),
            P("rep", "exp", None),
            P("exp", "rep", None),
            P("exp", "rep", None),
        ),
        check_vma=False,
    )
```

```python
import math

import jax
import jax.numpy as jnp
import numpy as np
from jax import lax
from jax.experimental import pallas as pl
from jax.experimental.pallas import tpu as pltpu
from jax.sharding import PartitionSpec as P

HEADS = 16
GELU_C = math.sqrt(2.0 / math.pi)
window_side = 8
margin_cells = 4
STORE_PARTS = 4
WEIGHT_PARTS, AHEAD, EARLY_G, NEARER = 2, 1, True, False
PAIR = 2
f32, bf16 = jnp.float32, jnp.bfloat16


class Windows:
    def __init__(self, tile_rows, tile_cols):
        def cut(size):
            parts = [margin_cells] + [window_side] * ((size - 2 * margin_cells) // window_side)
            return parts + [margin_cells]

        self.heights, self.widths = cut(tile_rows), cut(tile_cols)
        self.cells = window_side * window_side
        self.wins, start = [], 0
        for i, h in enumerate(self.heights):
            for j, w in enumerate(self.widths):
                sizes = (h * w, (window_side - h) * w, h * (window_side - w), (window_side - h) * (window_side - w))
                self.wins.append((i, j, start, sizes))
                start += h * w
        self.last = (len(self.heights) - 1, len(self.widths) - 1)

    def spots(self, tile_cols, tok):
        lane = lax.broadcasted_iota(jnp.int32, (1, tok), 1)
        rows, cols = lane // tile_cols, lax.rem(lane, tile_cols)

        def within(line, sizes):
            first, size, top = jnp.zeros_like(line), jnp.full_like(line, sizes[0]), 0
            for before, here in zip(sizes, sizes[1:]):
                top += before
                first, size = jnp.where(line >= top, top, first), jnp.where(line >= top, here, size)
            return first, size

        (top, height), (left, width) = within(rows, self.heights), within(cols, self.widths)
        return top * tile_cols + left * height + (rows - top) * width + cols - left

    def number(self, i, j):
        return i * len(self.widths) + j

    def segment(self, number, kind):
        sizes = self.wins[number][3]
        return number * self.cells + sum(sizes[:kind]), sizes[kind]

    def pieces(self, dv, dh):
        found = []
        for number, (i, j, _, _) in enumerate(self.wins):
            vertical = (dv == -1 and i == 0) or (dv == 1 and i == self.last[0])
            beside = (dh == -1 and j == 0) or (dh == 1 and j == self.last[1])
            if (dv and not vertical) or (dh and not beside):
                continue
            kind = (1 if dv else 0) + (2 if dh else 0)
            theirs = self.number(self.last[0] - i if dv else i, self.last[1] - j if dh else j)
            place, rows = self.segment(number, kind)
            found.append((self.wins[theirs][2], place, rows))
        return found


class Plan:
    def __init__(self, ranks, nearer):
        def handler(tile, pair):
            low = PAIR * pair
            if tile // PAIR == pair:
                return tile
            return (low if tile < low else low + 1) if nearer else low + tile % PAIR

        handled = [[t for t in range(ranks) if handler(t, p // PAIR) == p] for p in range(ranks)]
        self.tiles = [sorted(own, key=lambda t, p=p: (abs(t - p), t)) for p, own in enumerate(handled)]
        self.far = [[p for p in range(ranks) if p != t and t in self.tiles[p]] for t in range(ranks)]
        self.most = max(len(own) for own in self.tiles)
        self.sends = max(len(to) for to in self.far)
        self.counts = sorted({len(own) for own in self.tiles})
        assert len({len(to) for to in self.far}) == 1

    @staticmethod
    def pick(row, values):
        value = values[-1]
        if len(set(values)) > 1:
            for rank, other in enumerate(values[:-1]):
                value = jnp.where(row == rank, other, value)
        return value

    def handles(self, row, j):
        flags = [len(own) > j for own in self.tiles]
        return True if all(flags) else self.pick(row, [int(f) for f in flags]) == 1

    def has(self, row, count):
        return True if len(self.counts) == 1 else self.pick(row, [len(own) for own in self.tiles]) == count

    def origin(self, row, j):
        known = [(own[j], self.far[own[j]].index(p)) if len(own) > j else (0, 0) for p, own in enumerate(self.tiles)]
        return self.pick(row, [t for t, _ in known]), self.pick(row, [k for _, k in known])

    def goal(self, row, k):
        return (
            self.pick(row, [to[k] for to in self.far]),
            self.pick(row, [self.tiles[to[k]].index(t) for t, to in enumerate(self.far)]),
        )


def when(condition, body):
    if condition is True:
        body()
    else:
        pl.when(condition)(body)


SIDES = [(v, h) for v in (-1, 0, 1) for h in (-1, 0, 1) if (v, h) != (0, 0)]


def drain(ref, sem):
    pltpu.make_async_copy(ref, ref, sem).wait()


def dot_t(a, b):
    return lax.dot_general(a, b, (((1,), (1,)), ((), ())), preferred_element_type=f32)


def t_dot(a, b):
    return lax.dot_general(a, b, (((0,), (0,)), ((), ())), preferred_element_type=f32)


def dot(a, b):
    return jnp.dot(a, b, preferred_element_type=f32)


def layer_norm(values):
    average = jnp.mean(values, axis=-1, keepdims=True)
    centred = values - average
    spread = jnp.mean(centred * centred, axis=-1, keepdims=True)
    return centred * lax.rsqrt(spread + 1e-05)


def layer_kernel(
    wins, plan, ring, ranks, cap, tile_cols,
    tokens_hbm, cotangent_hbm, gate_hbm, route_hbm, w_qkv_hbm, w_proj_hbm, w_up_hbm, w_down_hbm,
    layer_out, input_grad, grad_up, grad_down,
    tokens, cotangent, gate, route, w_qkv, w_proj, w_up, w_down, grouped, ext, kv, queries, context, mixed, upstream, gate_col,
    marks, placers, held, slots, gathered, hidden, slopes, pre_grad, parts, back, sums, arrived, share, taken,
    load_sem, halo_send, halo_recv, mark_send, mark_recv, z_send, z_recv, a_send, a_recv,
    b_send, b_recv, w_send, w_recv, r_send, r_recv, g_send, g_recv,
):
    me, row = lax.axis_index("exp"), lax.axis_index("rep")
    tok, feature = tokens.shape
    units = w_up.shape[1]
    tiles, sends = plan.most, plan.sends
    buddy = row + 1 - 2 * lax.rem(row, 2)
    head_size = feature // HEADS

    def others(body):
        for j in range(1, tiles):
            when(plan.handles(row, j), lambda j=j: body(j))

    loads = {
        name: pltpu.make_async_copy(source, target, load_sem.at[i])
        for i, (name, source, target) in enumerate(
            (
                ("tokens", tokens_hbm, tokens),
                ("route", route_hbm, route),
                ("gate", gate_hbm, gate),
                ("cotangent", cotangent_hbm, cotangent),
                ("up", w_up_hbm, w_up.at[0]),
                ("qkv", w_qkv_hbm, w_qkv),
                ("down", w_down_hbm, w_down.at[0]),
                ("proj", w_proj_hbm, w_proj),
            )
        )
    }
    for load in loads.values():
        load.start()

    barrier = pltpu.get_barrier_semaphore()

    def near(v, h):
        conds = []
        if v:
            conds.append((row + v >= 0) & (row + v < ranks))
        if h:
            conds.append((me + h >= 0) & (me + h < ring))
        return conds[0] if len(conds) == 1 else conds[0] & conds[1]

    def greet_ring(step, carry):
        pl.semaphore_signal(barrier, device_id={"exp": lax.rem(me + step, ring)})
        return carry

    def greet_ranks(step, carry):
        pl.semaphore_signal(barrier, device_id={"rep": lax.rem(row + step, ranks)})
        return carry

    lax.fori_loop(1, ring, greet_ring, 0)
    lax.fori_loop(1, ranks, greet_ranks, 0)
    for v, h in SIDES:
        if v and h:
            @pl.when(near(v, h))
            def _():
                pl.semaphore_signal(barrier, device_id={"rep": row + v, "exp": me + h})

    spots = wins.spots(tile_cols, tok)
    perm = (lax.broadcasted_iota(jnp.int32, (tok, tok), 0) == spots).astype(f32).astype(bf16)
    loads["tokens"].wait()
    grouped[...] = dot(perm, tokens[...]).astype(bf16)
    for number, (i, j, start, sizes) in enumerate(wins.wins):
        ext[pl.ds(number * wins.cells, sizes[0]), :] = grouped[pl.ds(start, sizes[0]), :]
    for v, h in SIDES:
        @pl.when(jnp.logical_not(near(v, h)))
        def _():
            for _, place, rows in wins.pieces(v, h):
                ext[pl.ds(place, rows), :] = jnp.zeros((rows, feature), bf16)

    down = (row + ranks - 1) // ranks + (2 * ranks - 2 - row) // ranks
    across = (me + ring - 1) // ring + (2 * ring - 2 - me) // ring
    pl.semaphore_wait(barrier, ring - 1 + ranks - 1 + down * across)

    for index, (v, h) in enumerate(SIDES):
        @pl.when(near(v, h))
        def _():
            device = {"rep": row + v} if not h else {"exp": me + h} if not v else {"rep": row + v, "exp": me + h}
            for source, place, rows in wins.pieces(-v, -h):
                pltpu.make_async_remote_copy(
                    src_ref=grouped.at[pl.ds(source, rows)],
                    dst_ref=ext.at[pl.ds(place, rows)],
                    send_sem=halo_send.at[index],
                    recv_sem=halo_recv.at[len(SIDES) - 1 - index],
                    device_id=device,
                ).start()

    lanes = max(8, ring)
    loads["route"].wait()
    routes = route[0:1, :].astype(f32)
    match = (lax.broadcasted_iota(jnp.int32, (lanes, tok), 0).astype(f32) == routes).astype(f32)
    before = (
        lax.broadcasted_iota(jnp.int32, (tok, tok), 0) < lax.broadcasted_iota(jnp.int32, (tok, tok), 1)
    ).astype(f32).astype(bf16)
    earlier = dot(match.astype(bf16), before)
    ids = routes * cap + jnp.sum(match * earlier, axis=0, keepdims=True)
    marks[0] = jnp.broadcast_to(ids.astype(jnp.int32), marks.shape[1:])

    def send_marks():
        for k in range(sends):
            goal, place = plan.goal(row, k)
            pltpu.make_async_remote_copy(
                src_ref=marks.at[0],
                dst_ref=marks.at[place],
                send_sem=mark_send.at[k],
                recv_sem=mark_recv.at[place],
                device_id={"rep": goal},
            ).start()

    def send_tokens(t, source):
        for k in range(sends):
            goal, place = plan.goal(row, k)
            pltpu.make_async_remote_copy(
                src_ref=source,
                dst_ref=held.at[t, place],
                send_sem=z_send.at[t, k],
                recv_sem=z_recv.at[t, place],
                device_id={"rep": goal},
            ).start()

    def make_placer(j):
        slot_ids = lax.broadcasted_iota(jnp.int32, placers.shape[1:], 0)
        placers[j] = (slot_ids == marks[j, 0:1, :]).astype(f32).astype(bf16)

    def swap(source, target, send_sem, recv_sem):
        mine = pl.ds(pl.multiple_of(me * cap, 16), cap)

        def send(step, carry):
            peer = lax.rem(me + step, ring)
            pltpu.make_async_remote_copy(
                src_ref=source.at[pl.ds(pl.multiple_of(peer * cap, 16), cap)],
                dst_ref=target.at[mine],
                send_sem=send_sem,
                recv_sem=recv_sem,
                device_id={"exp": peer},
            ).start()
            return carry

        lax.fori_loop(1, ring, send, 0)
        pltpu.make_async_copy(source.at[mine], target.at[mine], recv_sem).start()

    def dispatch(t, j, values):
        slots[t, j] = dot(placers[j], values).astype(bf16)
        swap(slots.at[t, j], gathered.at[t, j], a_send.at[t, j], a_recv.at[t, j])


    def wait_halo():
        for index, (v, h) in enumerate(SIDES):
            @pl.when(near(v, h))
            def _():
                amount = sum(rows for _, _, rows in wins.pieces(v, h))
                drain(grouped.at[pl.ds(0, amount)], halo_recv.at[index])

    loads["gate"].wait()
    loads["cotangent"].wait()
    grid_row = lax.broadcasted_iota(jnp.int32, (tok, gate.shape[0]), 0) // tile_cols
    picks = (grid_row == lax.broadcasted_iota(jnp.int32, (tok, gate.shape[0]), 1)).astype(f32)
    gate_rows = lax.dot_general(
        picks, gate[...], (((1,), (0,)), ((), ())), precision=lax.Precision.HIGHEST, preferred_element_type=f32
    )
    grid_col = lax.rem(lax.broadcasted_iota(jnp.int32, (tok, tile_cols), 0), tile_cols)
    chosen = jnp.where(grid_col == lax.broadcasted_iota(jnp.int32, (tok, tile_cols), 1), gate_rows, 0.0)
    gate_col[...] = jnp.broadcast_to(jnp.sum(chosen, axis=1, keepdims=True), gate_col.shape)
    upstream[...] = (gate_col[:, 0:1] * cotangent[...].astype(f32)).astype(bf16)
    make_placer(0)

    loads["qkv"].wait()
    queries[...] = dot(grouped[...], w_qkv[:, :feature]).astype(bf16)
    if not EARLY_G:
        wait_halo()
    send_marks()
    send_tokens(0, upstream)
    dispatch(0, 0, upstream[...])

    chunk = units // WEIGHT_PARTS
    weights = [(m, p) for m in range(2) for p in range(WEIGHT_PARTS)]

    def weight_part(half, number):
        m, p = weights[number]
        return (w_up, w_down)[m].at[half, pl.ds(p * chunk, chunk)]

    def send_weights(numbers):
        for number in numbers:
            pltpu.make_async_remote_copy(
                src_ref=weight_part(0, number),
                dst_ref=weight_part(1, number),
                send_sem=w_send.at[number],
                recv_sem=w_recv.at[number],
                device_id={"rep": buddy},
            ).start()

    loads["up"].wait()
    loads["down"].wait()
    send_weights(range(AHEAD))
    if EARLY_G:
        wait_halo()
    kv[...] = dot(ext[...], w_qkv[:, feature:]).astype(bf16)
    key_lane = lax.broadcasted_iota(jnp.int32, (1, wins.cells), 1)
    group = 128 // head_size

    def attend(number):
        i, j, start, sizes = wins.wins[number]
        amount = sizes[0]
        absent = jnp.zeros((1, wins.cells), f32)
        v = -1 if i == 0 else 1 if i == wins.last[0] else 0
        h = -1 if j == 0 else 1 if j == wins.last[1] else 0
        for side in {(v, 0), (0, h), (v, h)} - {(0, 0)}:
            kind = (1 if side[0] else 0) + (2 if side[1] else 0)
            first = sum(sizes[:kind])
            inside = (key_lane >= first) & (key_lane < first + sizes[kind])
            missing = jnp.where(near(*side), 0.0, -1e30)
            absent = jnp.where(inside, missing, absent)
        lane = lax.broadcasted_iota(jnp.int32, (amount, 128), 1)
        keep = [((lane >= g * head_size) & (lane < (g + 1) * head_size)).astype(f32) for g in range(group)]
        mine, theirs = pl.ds(start, amount), pl.ds(number * wins.cells, wins.cells)
        for first in range(0, feature, 128):
            query = queries[mine, pl.ds(first, 128)]
            stacked = jnp.concatenate([query * k.astype(bf16) for k in keep], axis=0)
            scores = dot_t(stacked, kv[theirs, pl.ds(first, 128)]) * (1.0 / math.sqrt(head_size)) + absent
            weights = jnp.exp(scores - jnp.max(scores, axis=-1, keepdims=True))
            total = jnp.sum(weights, axis=-1, keepdims=True)
            probs = (weights * (1.0 / total)).astype(bf16)
            found = dot(probs, kv[theirs, pl.ds(feature + first, 128)])
            picked = sum(k * found[g * amount : (g + 1) * amount] for g, k in enumerate(keep))
            context[mine, pl.ds(first, 128)] = picked.astype(bf16)

    def bring(t, j):
        if t == 0:
            drain(marks.at[0], mark_recv.at[j])
            make_placer(j)
        drain(held.at[t, j], z_recv.at[t, j])
        dispatch(t, j, held[t, j])

    for number in range(len(wins.wins)):
        attend(number)

    loads["proj"].wait()
    attended = dot(context[...], w_proj[...])
    blended = (grouped[...].astype(f32) + layer_norm(attended)).astype(bf16)
    mixed[...] = t_dot(perm, blended).astype(bf16)
    send_tokens(1, mixed)
    dispatch(1, 0, mixed[...])
    send_weights(range(AHEAD, len(weights)))
    others(lambda j: bring(0, j))

    block = min(256, units)

    def arrive(j):
        for t in range(2):
            drain(gathered.at[t, j], a_recv.at[t, j])

    def rise(j, half):
        for first in range(0, units, block):
            pre = dot_t(gathered[1, j], w_up[half, pl.ds(first, block), :])
            square = pre * pre
            inner = jnp.tanh(GELU_C * (pre + 0.044715 * square * pre))
            hidden[j, :, pl.ds(half * units + first, block)] = (0.5 * pre * (1.0 + inner)).astype(bf16)
            slopes[j, :, pl.ds(first, block)] = 0.5 * (1.0 + inner) + 0.5 * pre * (1.0 - inner * inner) * GELU_C * (
                1.0 + 3.0 * 0.044715 * square
            )

    def fall(j, half):
        for first in range(0, units, block):
            flow = dot_t(gathered[0, j], w_down[half, pl.ds(first, block), :])
            spot = pl.ds(half * units + first, block)
            pre_grad[j, :, spot] = (flow * slopes[j, :, pl.ds(first, block)]).astype(bf16)

    def outputs(j):
        for t, (left, right) in enumerate(((hidden, w_down), (pre_grad, w_up))):
            total = dot(left[j, :, pl.ds(0, units)], right[0])
            for half in range(1, PAIR):
                total += dot(left[j, :, pl.ds(half * units, units)], right[half])
            parts[t, j] = total.astype(bf16)
            swap(parts.at[t, j], back.at[t, j], b_send.at[t, j], b_recv.at[t, j])

    def near_half(j):
        arrive(j)
        rise(j, 0)
        fall(j, 0)

    def gradient(t, half, count):
        left = (pre_grad, hidden)[t][0:count].reshape(count * hidden.shape[1], PAIR * units)
        right = gathered[1 - t, 0:count].reshape(count * hidden.shape[1], feature)
        return t_dot(left[:, half * units : (half + 1) * units], right)

    def give_gradient(t):
        for count in plan.counts:
            def partial(count=count):
                share[t] = gradient(t, 1, count).astype(bf16)

            when(plan.has(row, count), partial)
        pltpu.make_async_remote_copy(
            src_ref=share.at[t],
            dst_ref=taken.at[t],
            send_sem=g_send.at[t],
            recv_sem=g_recv.at[t],
            device_id={"rep": buddy},
        ).start()

    def await_weight(m):
        for number, (matrix, _) in enumerate(weights):
            if matrix == m:
                drain(weight_part(1, number), w_recv.at[number])

    near_half(0)
    others(lambda j: bring(1, j))
    others(near_half)
    await_weight(0)
    rise(0, 1)
    others(lambda j: rise(j, 1))
    give_gradient(1)
    await_weight(1)
    others(lambda j: fall(j, 1))
    fall(0, 1)
    give_gradient(0)
    others(outputs)
    outputs(0)

    def placed(t, j):
        drain(back.at[t, j], b_recv.at[t, j])
        return t_dot(placers[j], back[t, j])

    def give(j):
        goal, place = plan.origin(row, j)
        for t in range(2):
            sums[t, j] = placed(t, j).astype(bf16)
            pltpu.make_async_remote_copy(
                src_ref=sums.at[t, j],
                dst_ref=arrived.at[t, place],
                send_sem=r_send.at[t, j],
                recv_sem=r_recv.at[t, place],
                device_id={"rep": goal},
            ).start()

    for j in range(tiles - 1, 0, -1):
        when(plan.handles(row, j), lambda j=j: give(j))
    for count in plan.counts:
        def own_gradients(count=count):
            grad_up[...] = gradient(0, 0, count)
            grad_down[...] = gradient(1, 0, count)

        when(plan.has(row, count), own_gradients)

    def total_of(t):
        value = placed(t, 0)
        for k in range(sends):
            drain(arrived.at[t, k], r_recv.at[t, k])
            value += arrived[t, k].astype(f32)
        return value

    def finish_gradient(t):
        drain(taken.at[t], g_recv.at[t])
        out = (grad_up, grad_down)[t]
        out[...] = (out[...] + taken[t].astype(f32)) * (1.0 / ranks)

    finish_gradient(1)
    layer_out[...] = (mixed[...].astype(f32) + gate_col[:, 0:1] * total_of(0)).astype(bf16)
    input_grad[...] = total_of(1).astype(bf16)
    finish_gradient(0)

    for index, (v, h) in enumerate(SIDES):
        @pl.when(near(v, h))
        def _():
            amount = sum(rows for _, _, rows in wins.pieces(-v, -h))
            drain(grouped.at[pl.ds(0, amount)], halo_send.at[index])

    for number in range(len(weights)):
        drain(weight_part(0, number), w_send.at[number])
    for t in range(2):
        drain(share.at[t], g_send.at[t])
        for k in range(sends):
            drain(mixed, z_send.at[t, k])
    for k in range(sends):
        drain(marks.at[0], mark_send.at[k])

    def finish(j):
        for t in range(2):
            sent = slots.at[t, j, pl.ds(0, (ring - 1) * cap)]
            drain(sent, a_send.at[t, j])
            drain(sent, b_send.at[t, j])
            if j:
                drain(mixed, r_send.at[t, j])

    finish(0)
    others(finish)


def store(*values):
    count = len(values)
    pieces = [
        (i, pl.ds(first, v.shape[0] // STORE_PARTS))
        for i, v in enumerate(values)
        for first in range(0, v.shape[0], v.shape[0] // STORE_PARTS)
    ]

    def body(*refs):
        sems = refs[2 * count]
        copies = [
            pltpu.make_async_copy(refs[i].at[rows], refs[count + i].at[rows], sems.at[n])
            for n, (i, rows) in enumerate(pieces)
        ]
        for copy in copies:
            copy.start()
        for copy in copies:
            copy.wait()

    return pl.pallas_call(
        body,
        name="store",
        out_shape=tuple(jax.ShapeDtypeStruct(v.shape, v.dtype) for v in values),
        in_specs=[pl.BlockSpec(memory_space=pltpu.VMEM)] * count,
        out_specs=(pl.BlockSpec(memory_space=pl.ANY),) * count,
        scratch_shapes=[pltpu.SemaphoreType.DMA((len(pieces),))],
        compiler_params=pltpu.CompilerParams(vmem_limit_bytes=8 << 20),
    )(*values)


def per_device(ranks, ring, tokens, gate, route, cotangent, w_qkv, w_proj, w_up, w_down):
    tile_rows, tile_cols, feature = tokens.shape
    tok = tile_rows * tile_cols
    units = w_up.shape[1]
    capacity = max(2, 3 * tok // (2 * ring))
    capacity = -(-capacity // 16) * 16
    rows = ring * capacity
    wins = Windows(tile_rows, tile_cols)
    ext = len(wins.wins) * wins.cells

    vmem, hbm = pl.BlockSpec(memory_space=pltpu.VMEM), pl.BlockSpec(memory_space=pltpu.HBM)
    dma = pltpu.SemaphoreType.DMA
    def buffers_of(plan):
        tiles, sends = plan.most, plan.sends
        return [
            pltpu.VMEM((tok, feature), bf16),
            pltpu.VMEM((tok, feature), bf16),
            pltpu.VMEM(gate.shape, f32),
            pltpu.VMEM((1, tok), jnp.int32),
            pltpu.VMEM(w_qkv.shape, bf16),
            pltpu.VMEM(w_proj.shape, bf16),
            pltpu.VMEM((PAIR, units, feature), bf16),
            pltpu.VMEM((PAIR, units, feature), bf16),
            pltpu.VMEM((tok, feature), bf16),
            pltpu.VMEM((ext, feature), bf16),
            pltpu.VMEM((ext, 2 * feature), bf16),
            pltpu.VMEM((tok, feature), bf16),
            pltpu.VMEM((tok, feature), bf16),
            pltpu.VMEM((tok, feature), bf16),
            pltpu.VMEM((tok, feature), bf16),
            pltpu.VMEM((tok, 128), f32),
            pltpu.VMEM((tiles, 8, tok), jnp.int32),
            pltpu.VMEM((tiles, rows, tok), bf16),
            pltpu.VMEM((2, tiles, tok, feature), bf16),
            pltpu.VMEM((2, tiles, rows, feature), bf16),
            pltpu.VMEM((2, tiles, rows, feature), bf16),
            pltpu.VMEM((tiles, rows, PAIR * units), bf16),
            pltpu.VMEM((tiles, rows, units), f32),
            pltpu.VMEM((tiles, rows, PAIR * units), bf16),
            pltpu.VMEM((2, tiles, rows, feature), bf16),
            pltpu.VMEM((2, tiles, rows, feature), bf16),
            pltpu.VMEM((2, tiles, tok, feature), bf16),
            pltpu.VMEM((2, max(1, sends), tok, feature), bf16),
            pltpu.VMEM((2, units, feature), bf16),
            pltpu.VMEM((2, units, feature), bf16),
        ]

    def size_of(plan):
        return sum(math.prod(ref.shape) * jnp.dtype(ref.dtype).itemsize for ref in buffers_of(plan))

    plan = Plan(ranks, NEARER)
    if size_of(plan) > 44 << 20:
        plan = Plan(ranks, False)
    buffers, limit = buffers_of(plan), min(63 << 20, size_of(plan) + (16 << 20))
    tiles, sends = plan.most, max(1, plan.sends)
    semaphores = [
        dma((8,)),
        dma((len(SIDES),)),
        dma((len(SIDES),)),
        dma((sends,)),
        dma((tiles,)),
        dma((2, sends)),
        dma((2, tiles)),
        dma((2, tiles)),
        dma((2, tiles)),
        dma((2, tiles)),
        dma((2, tiles)),
        dma((2 * WEIGHT_PARTS,)),
        dma((2 * WEIGHT_PARTS,)),
        dma((2, tiles)),
        dma((2, sends)),
        dma((2,)),
        dma((2,)),
    ]

    def body(*refs):
        layer_kernel(wins, plan, ring, ranks, capacity, tile_cols, *refs)

    layer_out, input_grad, grad_up, grad_down = pl.pallas_call(
        body,
        name="layer",
        out_shape=(
            jax.ShapeDtypeStruct((tok, feature), bf16),
            jax.ShapeDtypeStruct((tok, feature), bf16),
            jax.ShapeDtypeStruct((units, feature), f32),
            jax.ShapeDtypeStruct((units, feature), f32),
        ),
        in_specs=[hbm] * 8,
        out_specs=(vmem,) * 4,
        scratch_shapes=buffers + semaphores,
        compiler_params=pltpu.CompilerParams(
            collective_id=0, has_side_effects=True, vmem_limit_bytes=limit
        ),
    )(
        *(
            pltpu.with_memory_space_constraint(array, pltpu.HBM)
            for array in (
                tokens.reshape(tok, feature),
                cotangent.reshape(tok, feature),
                gate,
                route.reshape(1, tok),
                w_qkv,
                w_proj,
                w_up[0],
                w_down[0],
            )
        )
    )
    layer_out, input_grad, grad_up, grad_down = store(layer_out, input_grad, grad_up, grad_down)
    return (
        layer_out.reshape(tile_rows, tile_cols, feature),
        input_grad.reshape(tile_rows, tile_cols, feature),
        grad_up[None],
        grad_down[None],
    )


def solution(mesh):
    ranks, ring = mesh.shape["rep"], mesh.shape["exp"]
    placed = (
        P("rep", "exp", None),
        P("rep", "exp"),
        P("rep", "exp", None, None),
        P("rep", "exp", None),
        P(),
        P(),
        P("exp", "rep", None),
        P("exp", "rep", None),
    )

    def device(*arrays):
        return per_device(ranks, ring, *arrays)

    return jax.shard_map(
        device,
        mesh=mesh,
        in_specs=placed,
        out_specs=(
            P("rep", "exp", None),
            P("rep", "exp", None),
            P("exp", "rep", None),
            P("exp", "rep", None),
        ),
        check_vma=False,
    )
```
